32 devices in a mesh: vid: 4 (over z), th: 4 (over x, core), tw: 2 (over y).
Axes of the slice: x: 2, y: 2, z: 4, core: 2. Of those that a mesh axis runs over, the one named last changes fastest.
Arguments:
- queries: bfloat16 [16, 32, 6, 3072], P('vid', 'th', 'tw'), parts along dimension 0, may hold values from -70 to 70
- video_kv: bfloat16 [2, 16, 32, 6, 3072], P(None, 'vid', 'th', 'tw'), parts along dimension 1, may hold values from -6 to 6
- text_kv: bfloat16 [2, 904, 3072], P(None, 'vid', 'tw'), parts along dimension 1, may hold values from -6 to 6
- time_embed: bfloat16 [2048], P('vid'), parts along dimension 0, may hold values from -6 to 6
- gate_weight: bfloat16 [512, 3072], P(None, 'tw'), may hold values from -0.25 to 0.25
- window_extent: int32 [48, 2], replicated, may hold values from 1 to 3
- tile_valid: int32 [16, 2, 2], P('vid'), parts along dimension 0, may hold values from 2 to 8, as said below
Outputs:
- gated: bfloat16 [16, 32, 6, 3072], P('vid', 'th', 'tw'), parts along dimension 0
The draws below stay inside these ranges and needn't reach their ends.
There are 4 independent parts, one for each index of `vid`. The reference program is written for one: setup_inputs(seed, part) draws one part's arguments, and reference() takes and returns one part's arrays. A program takes and returns all parts, laid end to end along the dimension named above; an argument that names none is the same for every part. Nothing has to cross between parts.
Inputs may be any that keep to these rules, and one draw needn't show every extreme that they name: Tile (i, j) holds tokens in its leading tile_valid[i, j, 0] of 8 rows and leading tile_valid[i, j, 1] of 3 columns; its other slots are padding. Some tile is full in every draw.
All inputs are finite; a program needn't handle non-finite values.
Results may differ from the reference program's by a relative error of at most 0.0063.
Values may be sent and summed in bfloat16 or wider, within the bound.
A program may use at most 128 MiB of HBM per device.

```python
import jax
import jax.numpy as jnp
from jax import lax

HEADS = 48
HEAD_DIM = 64
D = 3072
TXT = 226
TEMB = 512
FR = 4
TH_DEV = 8
TW_DEV = 3
HALO = 3
N_TH = 4
N_TW = 2


def clipped(rand_key, full_shape):
    return jnp.clip(jax.random.normal(rand_key, full_shape, jnp.float32), -6.0, 6.0)


def shared_fields(base_key):
    folded = jax.random.fold_in(base_key, 7301)
    key_q, key_k, key_v, key_tk, key_tv = jax.random.split(folded, 5)
    model_width = HEADS * HEAD_DIM
    full_shape = (FR, TH_DEV * N_TH, TW_DEV * N_TW, model_width)
    text_shape = (TXT, model_width)
    queries = clipped(key_q, full_shape)
    video_keys = clipped(key_k, full_shape)
    values = clipped(key_v, full_shape)
    text_keys = clipped(key_tk, text_shape)
    text_values = clipped(key_tv, text_shape)
    return (queries, jnp.stack([video_keys, values]), jnp.stack([text_keys, text_values]))


def draw_queries(key, part):
    return shared_fields(key)[0].astype(jnp.bfloat16)


def draw_video_kv(key, part):
    return shared_fields(key)[1].astype(jnp.bfloat16)


def draw_text_kv(key, part):
    return shared_fields(key)[2].astype(jnp.bfloat16)


def draw_tile_valid(key, part):
    folded = jax.random.fold_in(key, 5519)
    key_rows, key_cols, key_full = jax.random.split(folded, 3)
    valid_rows = jax.random.randint(key_rows, (N_TH, N_TW), 2, TH_DEV + 1)
    valid_cols = jax.random.randint(key_cols, (N_TH, N_TW), 2, TW_DEV + 1)
    full_tile = jax.random.randint(key_full, (), 0, N_TH * N_TW)
    chosen = jnp.arange(N_TH * N_TW).reshape(N_TH, N_TW) == full_tile
    valid_rows = jnp.where(chosen, TH_DEV, valid_rows)
    valid_cols = jnp.where(chosen, TW_DEV, valid_cols)
    return jnp.stack([valid_rows, valid_cols], axis=-1).astype(jnp.int32)


def set_ends(entries, own_key, smallest, largest):
    place = [jax.random.randint(jax.random.fold_in(own_key, axis), (), 0, length) for axis, length in enumerate(entries.shape)]
    main_axis = entries.shape.index(max(entries.shape))
    beside = place[:main_axis] + [(place[main_axis] + 1) % entries.shape[main_axis]] + place[main_axis + 1:]
    return entries.at[tuple(place)].set(smallest).at[tuple(beside)].set(largest)


def shard_levels(key, shape, shards, smallest, high):
    def one(axis_at, blocks):
        heights = jax.random.uniform(jax.random.fold_in(jax.random.fold_in(key, 6), axis_at), (blocks,), jnp.float32, smallest / len(shards), high / len(shards))
        return jnp.repeat(jnp.exp(heights), shape[axis_at] // blocks).reshape((-1,) + (1,) * (len(shape) - axis_at - 1))

    level = one(*shards[0])
    for cut in shards[1:]:
        level = level * one(*cut)
    return level


def normal_values(own_key, shape, spread, limit, cuts=(), held_as=jnp.bfloat16):
    level = shard_levels(own_key, shape, cuts, -0.22, 0.18) if cuts else 1.0
    values = jax.random.normal(own_key, shape, jnp.float32) * spread * level
    return jnp.minimum(jnp.maximum(values, -limit), limit).astype(held_as)


def setup_inputs(seed: int = 0, part: int = 0) -> dict:
    seeds = jax.random.split(jax.random.key(seed), 8)
    part_keys = jax.random.split(jax.random.fold_in(seeds[7], part), 8)
    queries = draw_queries(jax.random.fold_in(jax.random.fold_in(seeds[7], part), 71), part)
    video_kv = draw_video_kv(jax.random.fold_in(jax.random.fold_in(seeds[7], part), 71), part)
    text_kv = draw_text_kv(jax.random.fold_in(jax.random.fold_in(seeds[7], part), 71), part)
    time_embed = normal_values(part_keys[3], (TEMB,), 1.0, 6.0)
    gate_weight = normal_values(seeds[4], (TEMB, D), TEMB ** -0.5, 0.25, ((1, 2),))
    window_extent = set_ends(jax.random.randint(seeds[5], (HEADS, 2), 1, HALO + 1), jax.random.fold_in(seeds[5], 1), 1, HALO).astype(jnp.int32)
    tile_valid = draw_tile_valid(jax.random.fold_in(jax.random.fold_in(seeds[7], part), 71), part)
    return dict(queries=queries, video_kv=video_kv, text_kv=text_kv, time_embed=time_embed, gate_weight=gate_weight, window_extent=window_extent, tile_valid=tile_valid)


NEG = -1e30


def text_part(query_rows, text_keys, text_values, score_scale):
    scores = jnp.einsum("nhd,thd->nht", query_rows.astype(jnp.float32), text_keys.astype(jnp.float32)) * score_scale
    maximum = jnp.max(scores, axis=-1)
    exp_terms = jnp.exp(scores - maximum[..., None])
    totals = jnp.sum(exp_terms, axis=-1)
    rounded = lax.optimization_barrier(exp_terms.astype(jnp.bfloat16)).astype(jnp.float32)
    partial_value = jnp.einsum("nht,thd->nhd", rounded, text_values.astype(jnp.float32))
    return partial_value, maximum, totals


def video_part(query_rows, video_keys, video_values, key_ok, window_extent, frames, tile_rows, tile_cols, score_scale):
    count_q, head_count, head_depth = query_rows.shape
    span_rows = tile_rows + 2 * HALO
    span_cols = tile_cols + 2 * HALO
    row_gap = jnp.abs(jnp.arange(span_rows, dtype=jnp.int32)[None, :] - jnp.arange(tile_rows, dtype=jnp.int32)[:, None] - HALO)
    col_gap = jnp.abs(jnp.arange(span_cols, dtype=jnp.int32)[None, :] - jnp.arange(tile_cols, dtype=jnp.int32)[:, None] - HALO)
    near_row = row_gap[None] <= window_extent[:, 0][:, None, None]
    near_col = col_gap[None] <= window_extent[:, 1][:, None, None]
    allowed = near_row[:, None, :, None, None, :, None] & near_col[:, None, None, :, None, None, :] & key_ok[None, None, None, None, None, :, :]
    scores = jnp.einsum("nhd,khd->hnk", query_rows.astype(jnp.float32), video_keys.astype(jnp.float32)) * score_scale
    scores = jnp.where(allowed, scores.reshape(head_count, frames, tile_rows, tile_cols, frames, span_rows, span_cols), NEG)
    maximum = jnp.max(scores, axis=(4, 5, 6))
    exp_terms = jnp.where(allowed, jnp.exp(scores - maximum[..., None, None, None]), 0.0)
    totals = jnp.sum(exp_terms, axis=(4, 5, 6))
    rounded = lax.optimization_barrier(exp_terms.reshape(head_count, count_q, -1).astype(jnp.bfloat16)).astype(jnp.float32)
    partial_value = jnp.einsum("hnk,khd->nhd", rounded, video_values.astype(jnp.float32))
    return partial_value, maximum.reshape(head_count, count_q), totals.reshape(head_count, count_q)


def combine(video_out, video_max, video_total, text_out, text_max, text_total):
    max_v = video_max.T
    total_v = video_total.T
    joint_max = jnp.maximum(max_v, text_max)
    scale_v = jnp.exp(max_v - joint_max)
    scale_t = jnp.exp(text_max - joint_max)
    denom = total_v * scale_v + text_total * scale_t
    return (video_out * scale_v[..., None] + text_out * scale_t[..., None]) / denom[..., None]


def reference(queries, video_kv, text_kv, time_embed, gate_weight, window_extent, tile_valid):
    frames, grid_rows, grid_cols, model_width = queries.shape
    tile_rows = grid_rows // N_TH
    tile_cols = grid_cols // N_TW
    head_count = model_width // HEAD_DIM
    score_scale = HEAD_DIM ** -0.5
    span_rows = tile_rows + 2 * HALO
    span_cols = tile_cols + 2 * HALO
    mod_in = jax.nn.silu(time_embed.astype(jnp.float32)).astype(jnp.bfloat16)
    gate_full = jnp.dot(mod_in[None, :], gate_weight, preferred_element_type=jnp.float32)[0].astype(jnp.bfloat16)
    row_ids = jnp.arange(grid_rows, dtype=jnp.int32)
    col_ids = jnp.arange(grid_cols, dtype=jnp.int32)
    tile_limit = tile_valid[(row_ids // tile_rows)[:, None], (col_ids // tile_cols)[None, :]]
    token_ok = ((row_ids % tile_rows)[:, None] < tile_limit[..., 0]) & ((col_ids % tile_cols)[None, :] < tile_limit[..., 1])
    token_ok = token_ok.astype(jnp.int32)
    padded_kv = jnp.pad(video_kv, ((0, 0), (0, 0), (HALO, HALO), (HALO, HALO), (0, 0)))
    padded_ok = jnp.pad(token_ok, HALO)
    text_keys = text_kv[0].reshape(-1, head_count, HEAD_DIM)
    text_values = text_kv[1].reshape(-1, head_count, HEAD_DIM)

    def one_tile(tile_index):
        tile_row = tile_index // N_TW
        tile_col = tile_index % N_TW
        row_start = (tile_row * tile_rows).astype(jnp.int32)
        col_start = (tile_col * tile_cols).astype(jnp.int32)
        anchor = jnp.zeros((), jnp.int32)
        query_block = lax.dynamic_slice(queries, (anchor, row_start, col_start, anchor), (frames, tile_rows, tile_cols, model_width))
        kv_block = lax.dynamic_slice(padded_kv, (anchor, anchor, row_start, col_start, anchor), (2, frames, span_rows, span_cols, model_width))
        key_ok = lax.dynamic_slice(padded_ok, (row_start, col_start), (span_rows, span_cols)) > 0
        query_ok = lax.dynamic_slice(token_ok, (row_start, col_start), (tile_rows, tile_cols)) > 0
        query_rows = query_block.reshape(-1, head_count, HEAD_DIM)
        video_keys = kv_block[0].reshape(-1, head_count, HEAD_DIM)
        video_values = kv_block[1].reshape(-1, head_count, HEAD_DIM)
        video_out, video_max, video_total = video_part(query_rows, video_keys, video_values, key_ok, window_extent, frames, tile_rows, tile_cols, score_scale)
        text_out, text_max, text_total = text_part(query_rows, text_keys, text_values, score_scale)
        attended = combine(video_out, video_max, video_total, text_out, text_max, text_total)
        attended = attended.reshape(frames, tile_rows, tile_cols, model_width)
        result = jnp.where(query_ok[None, :, :, None], gate_full.astype(jnp.float32) * attended, 0.0)
        return result.astype(jnp.bfloat16)

    tile_out = lax.map(one_tile, jnp.arange(N_TH * N_TW, dtype=jnp.int32))
    tile_out = tile_out.reshape(N_TH, N_TW, frames, tile_rows, tile_cols, model_width)
    tile_out = jnp.transpose(tile_out, (2, 0, 3, 1, 4, 5))
    return tile_out.reshape(frames, grid_rows, grid_cols, model_width)
```

```python
import functools

import jax
import jax.numpy as jnp
import numpy as np
from jax import lax
from jax.experimental import pallas as pl
from jax.experimental.pallas import tpu as pltpu
from jax.sharding import PartitionSpec as P

HEAD_DIM = 64
HALO = 3
NEG = -1e30
FAR = 1 << 20
GROUP = 128
MESH = pl.DeviceIdType.MESH


def halo_rows(tile_rows, per_row):
    for rows in range(HALO, tile_rows + 1):
        if rows * per_row % 16 == 0:
            return rows
    return tile_rows


def dot_nt(a, b):
    return lax.dot_general(a, b, (((1,), (1,)), ((), ())), preferred_element_type=jnp.float32)


def kernel(
    dims,
    ext_in,
    valid_in,
    q_in,
    kv_in,
    text_in,
    time_in,
    gw_in,
    qmeta_in,
    kmeta_in,
    perm_in,
    out_ref,
    ext_ref,
    valid_ref,
    time_ref,
    qmeta,
    kmeta,
    perm,
    qbuf,
    kvbuf,
    packed,
    obuf,
    text_raw,
    text_ref,
    gw_ref,
    gate,
    row_gap,
    col_gap,
    pre_sem,
    loc_sem,
    send_sem,
    recv_sem,
    halo_send,
    halo_recv,
    out_send,
    out_recv,
):
    n_th, n_tw, chunks, lanes, tokens, halo, tile_cols, wide, flat = dims
    span = tokens + 2 * halo
    th = lax.axis_index("th")
    tw = lax.axis_index("tw")
    own = pl.ds(halo, tokens)
    heads_per_chunk = lanes // HEAD_DIM

    def peer(i):
        return lax.rem(tw + i, n_tw)

    def source(i):
        return lax.rem(tw + n_tw - i, n_tw)

    def piece(ref, j, c):
        if flat:
            return ref.at[..., pl.ds(pl.multiple_of((j * chunks + c) * lanes, lanes), lanes)]
        return ref.at[j, c]

    def remote(src, dst, ssem, rsem, where):
        return pltpu.make_async_remote_copy(
            src_ref=src, dst_ref=dst, send_sem=ssem, recv_sem=rsem, device_id=where, device_id_type=MESH
        )

    def kv_copy(c, i, slot):
        return remote(
            piece(kv_in, peer(i), c), kvbuf.at[c, slot, :, own, :], send_sem.at[c, i - 1, 0], recv_sem.at[c, i - 1, 0], {"tw": peer(i)}
        )

    def q_copy(c, i, slot):
        return remote(
            piece(q_in, peer(i), c), qbuf.at[c, slot], send_sem.at[c, i - 1, 1], recv_sem.at[c, i - 1, 1], {"tw": peer(i)}
        )

    def kv_local(c):
        return pltpu.make_async_copy(piece(kv_in, tw, c), kvbuf.at[c, tw, :, own, :], loc_sem.at[c, 0])

    def q_local(c):
        return pltpu.make_async_copy(piece(q_in, tw, c), qbuf.at[c, tw], loc_sem.at[c, 1])

    def halo_up(c, landing):
        dst = pl.ds(halo + tokens, halo)
        return remote(
            packed.at[c, :, :, pl.ds(0, halo), :], kvbuf.at[c, :, :, dst, :], halo_send.at[c, 0], halo_recv.at[c, 0], {"th": th - 1 + landing}
        )

    def halo_down(c, landing):
        dst = pl.ds(0, halo)
        return remote(
            packed.at[c, :, :, pl.ds(halo, halo), :], kvbuf.at[c, :, :, dst, :], halo_send.at[c, 1], halo_recv.at[c, 1], {"th": th + 1 - landing}
        )

    def out_copy(c, i, slot):
        return remote(obuf.at[c, peer(i)], piece(out_ref, slot, c), out_send.at[c, i - 1], out_recv.at[c, i - 1], {"tw": peer(i)})

    def out_local(c):
        return pltpu.make_async_copy(obuf.at[c, tw], piece(out_ref, tw, c), loc_sem.at[c, 2])

    has_up = th > 0
    has_down = th < n_th - 1

    barrier = pltpu.get_barrier_semaphore()
    for i in range(1, n_tw):
        pl.semaphore_signal(barrier, inc=1, device_id={"tw": peer(i)}, device_id_type=MESH)

    @pl.when(has_up)
    def _():
        pl.semaphore_signal(barrier, inc=1, device_id={"th": th - 1}, device_id_type=MESH)

    @pl.when(has_down)
    def _():
        pl.semaphore_signal(barrier, inc=1, device_id={"th": th + 1}, device_id_type=MESH)

    pl.semaphore_wait(barrier, n_tw - 1 + has_up.astype(jnp.int32) + has_down.astype(jnp.int32))

    for c in range(chunks):
        for i in range(1, n_tw):
            kv_copy(c, i, tw).start()
    for c in range(chunks):
        for i in range(1, n_tw):
            q_copy(c, i, tw).start()

    gw_load = pltpu.make_async_copy(gw_in, gw_ref, pre_sem.at[0])
    text_load = pltpu.make_async_copy(text_in, text_raw, pre_sem.at[1])
    for c in range(chunks):
        kv_local(c).start()
        q_local(c).start()
    small = [
        pltpu.make_async_copy(src, dst, pre_sem.at[2 + k])
        for k, (src, dst) in enumerate(
            [
                (ext_in, ext_ref),
                (valid_in, valid_ref),
                (time_in, time_ref),
                (qmeta_in, qmeta),
                (kmeta_in, kmeta),
                (perm_in, perm),
            ]
        )
    ]
    for load in small:
        load.start()
    gw_load.start()
    text_load.start()

    @pl.when(jnp.logical_not(has_up))
    def _():
        kvbuf[:, :, :, pl.ds(0, halo), :] = jnp.zeros((chunks, n_tw, 2, halo, lanes), kvbuf.dtype)

    @pl.when(jnp.logical_not(has_down))
    def _():
        kvbuf[:, :, :, pl.ds(halo + tokens, halo), :] = jnp.zeros((chunks, n_tw, 2, halo, lanes), kvbuf.dtype)

    def find_gate():
        time = time_ref[...].astype(jnp.float32)
        mod_in = (time / (1.0 + jnp.exp(-time))).astype(jnp.bfloat16)
        gw_load.wait()
        depth = mod_in.shape[1]
        gate_vec = jnp.zeros((1, chunks * lanes), jnp.float32)
        for k in range(mod_in.shape[0]):
            gate_vec = gate_vec + jnp.dot(
                mod_in[k : k + 1], gw_ref[k * depth : (k + 1) * depth], preferred_element_type=jnp.float32
            )
        gate_vec = gate_vec.astype(jnp.bfloat16).astype(jnp.float32)
        for c in range(chunks):
            gate[c] = gate_vec[:, c * lanes : (c + 1) * lanes]

    for load in small:
        load.wait()

    reach = -(-HALO // tile_cols)

    def first_tile(t):
        return jnp.clip(t - reach, 0, n_tw - wide)

    q_row = qmeta[:, 0:1]
    q_col = qmeta[:, 1:2]
    k_row = kmeta[0:1, :]
    k_band = kmeta[1:2, :]
    k_local = kmeta[2:3, :]
    k_col = kmeta[3:4, :]
    above = jnp.maximum(th - 1, 0)
    below = jnp.minimum(th + 1, n_th - 1)

    def distances(t, carry):
        start = first_tile(t)
        for j in range(wide):
            tc = start + j
            limits = []
            for what in range(2):
                up = jnp.where(has_up, valid_ref[tc, what, above], 0)
                mid = valid_ref[tc, what, th]
                down = jnp.where(has_down, valid_ref[tc, what, below], 0)
                limits.append(jnp.where(k_band == 0, up, jnp.where(k_band == 1, mid, down)))
            bad = jnp.where((k_local < limits[0]) & (k_col < limits[1]), 0, FAR)
            row_gap[t, :, pl.ds(j * span, span)] = jnp.abs(k_row - q_row) + bad
            col_gap[t, :, pl.ds(j * span, span)] = jnp.abs(k_col + (tc - t) * tile_cols - q_col)
        return carry

    lax.fori_loop(0, n_tw, distances, 0)
    find_gate()
    text_load.wait()
    for s in range(2):
        text_ref[s] = text_raw[:, s, :]

    def attend(c, t):
        start = first_tile(t)
        q_ok = (q_row < valid_ref[t, 0, th]) & (q_col < valid_ref[t, 1, th])
        rows_apart = row_gap[t]
        cols_apart = col_gap[t]
        for low in range(0, lanes, GROUP):
            width = min(GROUP, lanes - low)
            count = width // HEAD_DIM
            part = pl.ds(low, width)
            q = qbuf[c, t, :, part]
            keys = kvbuf[c, pl.ds(start, wide), 0, :, part].reshape(wide * span, width)
            values = kvbuf[c, pl.ds(start, wide), 1, :, part].reshape(wide * span, width)
            if chunks == 1:
                at = part
            else:
                at = pl.ds(pl.multiple_of(c * lanes + low, GROUP), width)
            t_keys = text_ref[0, :, at]
            t_values = text_ref[1, :, at]
            lane = lax.broadcasted_iota(jnp.int32, (1, width), 1)
            stacked = []
            for s in range(count):
                mine = (lane >= s * HEAD_DIM) & (lane < (s + 1) * HEAD_DIM)
                stacked.append(q * jnp.where(mine, HEAD_DIM ** -0.5, 0.0).astype(jnp.bfloat16))
            q_all = jnp.concatenate(stacked, axis=0) if count > 1 else stacked[0]
            scores = dot_nt(q_all, keys)
            t_scores = dot_nt(q_all, t_keys)
            weights, t_weights, inverse = [], [], []
            for s in range(count):
                head = tw * (chunks * heads_per_chunk) + c * heads_per_chunk + low // HEAD_DIM + s
                allowed = (rows_apart <= ext_ref[0, head]) & (cols_apart <= ext_ref[1, head])
                sv = jnp.where(allowed, scores[s * tokens : (s + 1) * tokens], NEG)
                st = t_scores[s * tokens : (s + 1) * tokens]
                top = jnp.maximum(jnp.max(sv, axis=-1, keepdims=True), jnp.max(st, axis=-1, keepdims=True))
                ev = jnp.exp(sv - top)
                et = jnp.exp(st - top)
                inverse.append(1.0 / (jnp.sum(ev, axis=-1, keepdims=True) + jnp.sum(et, axis=-1, keepdims=True)))
                weights.append(ev.astype(jnp.bfloat16))
                t_weights.append(et.astype(jnp.bfloat16))
            w_all = jnp.concatenate(weights, axis=0) if count > 1 else weights[0]
            tw_all = jnp.concatenate(t_weights, axis=0) if count > 1 else t_weights[0]
            mixed = jnp.dot(w_all, values, preferred_element_type=jnp.float32) + jnp.dot(
                tw_all, t_values, preferred_element_type=jnp.float32
            )
            result = mixed[0:tokens] * inverse[0]
            for s in range(1, count):
                result = jnp.where(lane >= s * HEAD_DIM, mixed[s * tokens : (s + 1) * tokens] * inverse[s], result)
            result = result * gate[c, :, part]
            obuf[c, t, :, part] = jnp.where(q_ok, result, 0.0).astype(jnp.bfloat16)

    lag = min(2, chunks)

    def step(at, carry):
        @pl.when(at < chunks)
        def _():
            kv_local(at).wait()
            for i in range(1, n_tw):
                kv_copy(at, i, source(i)).wait_recv()

            def pack(j, inner):
                for s in range(2):
                    rows = jnp.dot(perm[...], kvbuf[at, j, s, own, :], preferred_element_type=jnp.float32)
                    packed[at, j, s] = rows.astype(jnp.bfloat16)
                return inner

            lax.fori_loop(0, n_tw, pack, 0)

            @pl.when(has_up)
            def _():
                halo_up(at, 0).start()

            @pl.when(has_down)
            def _():
                halo_down(at, 0).start()

        @pl.when((at >= lag) & (at < chunks + lag))
        def _():
            c = at - lag
            q_local(c).wait()

            @pl.when(has_down)
            def _():
                halo_up(c, 2).wait_recv()

            @pl.when(has_up)
            def _():
                halo_down(c, 2).wait_recv()

        @pl.when(at >= chunks)
        def _():
            c = at - chunks
            for i in range(1, n_tw):
                q_copy(c, i, source(i)).wait_recv()

            def one(i, inner):
                attend(c, peer(i))
                return inner

            lax.fori_loop(1, n_tw, one, 0)
            for i in range(1, n_tw):
                out_copy(c, i, tw).start()

        @pl.when((at >= lag) & (at < chunks + lag))
        def _():
            attend(at - lag, tw)
            out_local(at - lag).start()

        return carry

    lax.fori_loop(0, chunks + max(chunks, lag), step, 0)

    for c in range(chunks):
        for i in range(1, n_tw):
            kv_copy(c, i, tw).wait_send()
            q_copy(c, i, tw).wait_send()
            out_copy(c, i, tw).wait_send()
            out_copy(c, i, source(i)).wait_recv()
        out_local(c).wait()

        @pl.when(has_up)
        def _():
            halo_up(c, 0).wait_send()

        @pl.when(has_down)
        def _():
            halo_down(c, 0).wait_send()


def body(sizes, queries, video_kv, text_kv, time_embed, gate_weight, window_extent, tile_valid):
    n_th, n_tw = sizes
    frames, tile_rows, tile_cols, model_width = queries.shape
    per_row = frames * tile_cols
    tokens = tile_rows * per_row
    rows = halo_rows(tile_rows, per_row)
    halo = rows * per_row
    span = tokens + 2 * halo
    own_width = model_width // n_tw
    lanes = 2 * GROUP if own_width % (2 * GROUP) == 0 else own_width
    chunks = own_width // lanes
    wide = min(n_tw, 2 * -(-HALO // tile_cols) + 1)

    flat = lanes % GROUP == 0

    q = queries.transpose(0, 2, 1, 3).reshape(tokens, model_width)
    kv = video_kv.transpose(0, 1, 3, 2, 4).reshape(2, tokens, model_width)
    out_form = (tokens, model_width)
    if not flat:
        q = q.reshape(tokens, n_tw, chunks, lanes).transpose(1, 2, 0, 3)
        kv = kv.reshape(2, tokens, n_tw, chunks, lanes).transpose(2, 3, 0, 1, 4)
        out_form = (n_tw, chunks, tokens, lanes)

    ids = np.arange(tokens)
    q_col, q_row = ids // tile_rows % tile_cols, ids % tile_rows
    q_meta = np.stack([q_row, q_col], axis=1).astype(np.int32)
    h_ids = np.arange(halo)
    h_block, h_row = h_ids // rows, h_ids % rows
    k_row = np.concatenate([h_row - rows, q_row, h_row + tile_rows])
    k_col = np.concatenate([h_block % tile_cols, q_col, h_block % tile_cols])
    band = np.floor_divide(k_row, tile_rows) + 1
    k_meta = np.zeros((8, span), np.int32)
    k_meta[0], k_meta[1] = k_row, band
    k_meta[2], k_meta[3] = k_row - (band - 1) * tile_rows, k_col
    picks = np.concatenate([h_block * tile_rows + h_row, h_block * tile_rows + h_row + tile_rows - rows])
    perm = (picks[:, None] == ids[None, :]).astype(np.float32)
    depth = GROUP if time_embed.shape[0] % GROUP == 0 else time_embed.shape[0]

    hbm = pl.BlockSpec(memory_space=pltpu.HBM)
    others = max(n_tw - 1, 1)
    dma = pltpu.SemaphoreType.DMA
    out = pl.pallas_call(
        functools.partial(kernel, (n_th, n_tw, chunks, lanes, tokens, halo, tile_cols, wide, flat)),
        out_shape=pltpu.VMEM(out_form, jnp.bfloat16),
        in_specs=[hbm] * 10,
        out_specs=hbm,
        scratch_shapes=[
            pltpu.SMEM((2, window_extent.shape[0]), jnp.int32),
            pltpu.SMEM((n_tw, 2, n_th), jnp.int32),
            pltpu.VMEM((time_embed.shape[0] // depth, depth), jnp.bfloat16),
            pltpu.VMEM(q_meta.shape, jnp.int32),
            pltpu.VMEM(k_meta.shape, jnp.int32),
            pltpu.VMEM(perm.shape, jnp.bfloat16),
            pltpu.VMEM((chunks, n_tw, tokens, lanes), jnp.bfloat16),
            pltpu.VMEM((chunks, n_tw, 2, span, lanes), jnp.bfloat16),
            pltpu.VMEM((chunks, n_tw, 2, 2 * halo, lanes), jnp.bfloat16),
            pltpu.VMEM((chunks, n_tw, tokens, lanes), jnp.bfloat16),
            pltpu.VMEM((text_kv.shape[1], 2, text_kv.shape[2]), jnp.bfloat16),
            pltpu.VMEM(text_kv.shape, jnp.bfloat16),
            pltpu.VMEM(gate_weight.shape, jnp.bfloat16),
            pltpu.VMEM((chunks, 1, lanes), jnp.float32),
            pltpu.VMEM((n_tw, tokens, wide * span), jnp.int32),
            pltpu.VMEM((n_tw, tokens, wide * span), jnp.int32),
            dma((8,)),
            dma((chunks, 3)),
            dma((chunks, others, 2)),
            dma((chunks, others, 2)),
            dma((chunks, 2)),
            dma((chunks, 2)),
            dma((chunks, others)),
            dma((chunks, others)),
        ],
        compiler_params=pltpu.CompilerParams(
            collective_id=0, has_side_effects=True, vmem_limit_bytes=56 * 1024 * 1024
        ),
    )(
        window_extent.T,
        tile_valid.transpose(1, 2, 0),
        q,
        kv,
        text_kv.transpose(1, 0, 2),
        time_embed.reshape(-1, depth),
        gate_weight,
        jnp.asarray(q_meta),
        jnp.asarray(k_meta),
        jnp.asarray(perm, jnp.bfloat16),
    )
    if not flat:
        out = out.transpose(2, 0, 1, 3)
    return out.reshape(frames, tile_cols, tile_rows, model_width).transpose(0, 2, 1, 3)


def solution(mesh):
    placed = (
        P("vid", "th", "tw", None),
        P(None, "vid", "th", "tw", None),
        P(None, "vid", "tw"),
        P("vid"),
        P(None, "tw"),
        P(),
        P("vid", None, None),
    )
    return jax.shard_map(
        functools.partial(body, (mesh.shape["th"], mesh.shape["tw"])),
        mesh=mesh,
        in_specs=placed,
        out_specs=P("vid", "th", "tw", None),
        check_vma=False,
    )
```

```python
import functools

import jax
import jax.numpy as jnp
import numpy as np
from jax import lax
from jax.experimental import pallas as pl
from jax.experimental.pallas import tpu as pltpu
from jax.sharding import PartitionSpec as P

HEAD_DIM = 64
HALO = 3
NEG = -1e30
FAR = 1 << 20
GROUP = 128
MESH = pl.DeviceIdType.MESH


def halo_rows(tile_rows, per_row):
    for rows in range(HALO, tile_rows + 1):
        if rows * per_row % 16 == 0:
            return rows
    return tile_rows


def dot_nt(a, b):
    return lax.dot_general(a, b, (((1,), (1,)), ((), ())), preferred_element_type=jnp.float32)


def kernel(
    dims,
    ext_in,
    valid_in,
    q_in,
    kv_in,
    text_in,
    time_in,
    gw_in,
    qmeta_in,
    kmeta_in,
    perm_in,
    out_ref,
    ext_ref,
    valid_ref,
    time_ref,
    qmeta,
    kmeta,
    perm,
    qbuf,
    kvbuf,
    packed,
    obuf,
    text_raw,
    text_ref,
    gw_ref,
    gate,
    row_gap,
    col_gap,
    pre_sem,
    loc_sem,
    send_sem,
    recv_sem,
    halo_send,
    halo_recv,
    out_send,
    out_recv,
):
    n_th, n_tw, chunks, lanes, tokens, halo, tile_cols, wide, flat = dims
    span = tokens + 2 * halo
    th = lax.axis_index("th")
    tw = lax.axis_index("tw")
    own = pl.ds(halo, tokens)
    heads_per_chunk = lanes // HEAD_DIM

    def peer(i):
        return lax.rem(tw + i, n_tw)

    def source(i):
        return lax.rem(tw + n_tw - i, n_tw)

    def piece(ref, j, c):
        if flat:
            return ref.at[..., pl.ds(pl.multiple_of((j * chunks + c) * lanes, lanes), lanes)]
        return ref.at[j, c]

    def remote(src, dst, ssem, rsem, where):
        return pltpu.make_async_remote_copy(
            src_ref=src, dst_ref=dst, send_sem=ssem, recv_sem=rsem, device_id=where, device_id_type=MESH
        )

    def kv_copy(c, i, slot):
        return remote(
            piece(kv_in, peer(i), c), kvbuf.at[c, slot, :, own, :], send_sem.at[c, i - 1, 0], recv_sem.at[c, i - 1, 0], {"tw": peer(i)}
        )

    def q_copy(c, i, slot):
        return remote(
            piece(q_in, peer(i), c), qbuf.at[c, slot], send_sem.at[c, i - 1, 1], recv_sem.at[c, i - 1, 1], {"tw": peer(i)}
        )

    def kv_local(c):
        return pltpu.make_async_copy(piece(kv_in, tw, c), kvbuf.at[c, tw, :, own, :], loc_sem.at[c, 0])

    def q_local(c):
        return pltpu.make_async_copy(piece(q_in, tw, c), qbuf.at[c, tw], loc_sem.at[c, 1])

    def halo_up(c, landing):
        dst = pl.ds(halo + tokens, halo)
        return remote(
            packed.at[c, :, :, pl.ds(0, halo), :], kvbuf.at[c, :, :, dst, :], halo_send.at[c, 0], halo_recv.at[c, 0], {"th": th - 1 + landing}
        )

    def halo_down(c, landing):
        dst = pl.ds(0, halo)
        return remote(
            packed.at[c, :, :, pl.ds(halo, halo), :], kvbuf.at[c, :, :, dst, :], halo_send.at[c, 1], halo_recv.at[c, 1], {"th": th + 1 - landing}
        )

    def out_copy(c, i, slot):
        return remote(obuf.at[c, peer(i)], piece(out_ref, slot, c), out_send.at[c, i - 1], out_recv.at[c, i - 1], {"tw": peer(i)})

    def out_local(c):
        return pltpu.make_async_copy(obuf.at[c, tw], piece(out_ref, tw, c), loc_sem.at[c, 2])

    has_up = th > 0
    has_down = th < n_th - 1

    barrier = pltpu.get_barrier_semaphore()
    for i in range(1, n_tw):
        pl.semaphore_signal(barrier, inc=1, device_id={"tw": peer(i)}, device_id_type=MESH)

    @pl.when(has_up)
    def _():
        pl.semaphore_signal(barrier, inc=1, device_id={"th": th - 1}, device_id_type=MESH)

    @pl.when(has_down)
    def _():
        pl.semaphore_signal(barrier, inc=1, device_id={"th": th + 1}, device_id_type=MESH)

    pl.semaphore_wait(barrier, n_tw - 1 + has_up.astype(jnp.int32) + has_down.astype(jnp.int32))

    for c in range(chunks):
        for i in range(1, n_tw):
            kv_copy(c, i, tw).start()
    for c in range(chunks):
        for i in range(1, n_tw):
            q_copy(c, i, tw).start()

    gw_load = pltpu.make_async_copy(gw_in, gw_ref, pre_sem.at[0])
    text_load = pltpu.make_async_copy(text_in, text_raw, pre_sem.at[1])
    for c in range(chunks):
        kv_local(c).start()
        q_local(c).start()
    small = [
        pltpu.make_async_copy(src, dst, pre_sem.at[2 + k])
        for k, (src, dst) in enumerate(
            [
                (ext_in, ext_ref),
                (valid_in, valid_ref),
                (time_in, time_ref),
                (qmeta_in, qmeta),
                (kmeta_in, kmeta),
                (perm_in, perm),
            ]
        )
    ]
    for load in small:
        load.start()
    gw_load.start()
    text_load.start()

    @pl.when(jnp.logical_not(has_up))
    def _():
        kvbuf[:, :, :, pl.ds(0, halo), :] = jnp.zeros((chunks, n_tw, 2, halo, lanes), kvbuf.dtype)

    @pl.when(jnp.logical_not(has_down))
    def _():
        kvbuf[:, :, :, pl.ds(halo + tokens, halo), :] = jnp.zeros((chunks, n_tw, 2, halo, lanes), kvbuf.dtype)

    def find_gate():
        time = time_ref[...].astype(jnp.float32)
        mod_in = (time / (1.0 + jnp.exp(-time))).astype(jnp.bfloat16)
        gw_load.wait()
        depth = mod_in.shape[1]
        gate_vec = jnp.zeros((1, chunks * lanes), jnp.float32)
        for k in range(mod_in.shape[0]):
            gate_vec = gate_vec + jnp.dot(
                mod_in[k : k + 1], gw_ref[k * depth : (k + 1) * depth], preferred_element_type=jnp.float32
            )
        gate_vec = gate_vec.astype(jnp.bfloat16).astype(jnp.float32)
        for c in range(chunks):
            gate[c] = gate_vec[:, c * lanes : (c + 1) * lanes]

    for load in small:
        load.wait()

    reach = -(-HALO // tile_cols)

    def first_tile(t):
        return jnp.clip(t - reach, 0, n_tw - wide)

    q_row = qmeta[:, 0:1]
    q_col = qmeta[:, 1:2]
    k_row = kmeta[0:1, :]
    k_band = kmeta[1:2, :]
    k_local = kmeta[2:3, :]
    k_col = kmeta[3:4, :]
    above = jnp.maximum(th - 1, 0)
    below = jnp.minimum(th + 1, n_th - 1)

    def distances(t, carry):
        start = first_tile(t)
        for j in range(wide):
            tc = start + j
            limits = []
            for what in range(2):
                up = jnp.where(has_up, valid_ref[tc, what, above], 0)
                mid = valid_ref[tc, what, th]
                down = jnp.where(has_down, valid_ref[tc, what, below], 0)
                limits.append(jnp.where(k_band == 0, up, jnp.where(k_band == 1, mid, down)))
            bad = jnp.where((k_local < limits[0]) & (k_col < limits[1]), 0, FAR)
            row_gap[t, :, pl.ds(j * span, span)] = jnp.abs(k_row - q_row) + bad
            col_gap[t, :, pl.ds(j * span, span)] = jnp.abs(k_col + (tc - t) * tile_cols - q_col)
        return carry

    lax.fori_loop(0, n_tw, distances, 0)
    find_gate()
    text_load.wait()

    def attend(c, t):
        start = first_tile(t)
        q_ok = (q_row < valid_ref[t, 0, th]) & (q_col < valid_ref[t, 1, th])
        rows_apart = row_gap[t]
        cols_apart = col_gap[t]
        for low in range(0, lanes, GROUP):
            width = min(GROUP, lanes - low)
            count = width // HEAD_DIM
            part = pl.ds(low, width)
            q = qbuf[c, t, :, part]
            keys = kvbuf[c, pl.ds(start, wide), 0, :, part].reshape(wide * span, width)
            values = kvbuf[c, pl.ds(start, wide), 1, :, part].reshape(wide * span, width)
            t_keys = text_ref[c, 0, :, part]
            t_values = text_ref[c, 1, :, part]
            lane = lax.broadcasted_iota(jnp.int32, (1, width), 1)
            stacked = []
            for s in range(count):
                mine = (lane >= s * HEAD_DIM) & (lane < (s + 1) * HEAD_DIM)
                stacked.append(q * jnp.where(mine, HEAD_DIM ** -0.5, 0.0).astype(jnp.bfloat16))
            q_all = jnp.concatenate(stacked, axis=0) if count > 1 else stacked[0]
            scores = dot_nt(q_all, keys)
            t_scores = dot_nt(q_all, t_keys)
            weights, t_weights, inverse = [], [], []
            for s in range(count):
                head = tw * (chunks * heads_per_chunk) + c * heads_per_chunk + low // HEAD_DIM + s
                allowed = (rows_apart <= ext_ref[0, head]) & (cols_apart <= ext_ref[1, head])
                sv = jnp.where(allowed, scores[s * tokens : (s + 1) * tokens], NEG)
                st = t_scores[s * tokens : (s + 1) * tokens]
                top = jnp.maximum(jnp.max(sv, axis=-1, keepdims=True), jnp.max(st, axis=-1, keepdims=True))
                ev = jnp.exp(sv - top)
                et = jnp.exp(st - top)
                inverse.append(1.0 / (jnp.sum(ev, axis=-1, keepdims=True) + jnp.sum(et, axis=-1, keepdims=True)))
                weights.append(ev.astype(jnp.bfloat16))
                t_weights.append(et.astype(jnp.bfloat16))
            w_all = jnp.concatenate(weights, axis=0) if count > 1 else weights[0]
            tw_all = jnp.concatenate(t_weights, axis=0) if count > 1 else t_weights[0]
            mixed = jnp.dot(w_all, values, preferred_element_type=jnp.float32) + jnp.dot(
                tw_all, t_values, preferred_element_type=jnp.float32
            )
            result = mixed[0:tokens] * inverse[0]
            for s in range(1, count):
                result = jnp.where(lane >= s * HEAD_DIM, mixed[s * tokens : (s + 1) * tokens] * inverse[s], result)
            result = result * gate[c, :, part]
            obuf[c, t, :, part] = jnp.where(q_ok, result, 0.0).astype(jnp.bfloat16)

    lag = min(2, chunks)

    def halos_here(c):
        @pl.when(has_down)
        def _():
            halo_up(c, 2).wait_recv()

        @pl.when(has_up)
        def _():
            halo_down(c, 2).wait_recv()

    def step(at, carry):
        @pl.when(at < chunks)
        def _():
            kv_local(at).wait()
            for i in range(1, n_tw):
                kv_copy(at, i, source(i)).wait_recv()

            def pack(j, inner):
                for s in range(2):
                    rows = jnp.dot(perm[...], kvbuf[at, j, s, own, :], preferred_element_type=jnp.float32)
                    packed[at, j, s] = rows.astype(jnp.bfloat16)
                return inner

            lax.fori_loop(0, n_tw, pack, 0)

            @pl.when(has_up)
            def _():
                halo_up(at, 0).start()

            @pl.when(has_down)
            def _():
                halo_down(at, 0).start()

            mine = slice(None) if chunks == 1 else pl.ds(pl.multiple_of(at * lanes, lanes), lanes)
            for s in range(2):
                text_ref[at, s] = text_raw[:, s, mine]

        @pl.when((at >= chunks) & (at < 2 * chunks))
        def _():
            c = at - chunks

            @pl.when(c >= chunks - lag)
            def _():
                halos_here(c)

            for i in range(1, n_tw):
                q_copy(c, i, source(i)).wait_recv()

            def one(i, inner):
                attend(c, peer(i))
                return inner

            lax.fori_loop(1, n_tw, one, 0)
            for i in range(1, n_tw):
                out_copy(c, i, tw).start()

        @pl.when(((at >= lag) & (at < chunks)) | (at >= 2 * chunks))
        def _():
            c = jnp.where(at < chunks, at - lag, at - chunks - lag)

            @pl.when(at < chunks)
            def _():
                halos_here(c)

            q_local(c).wait()
            attend(c, tw)
            out_local(c).start()

        return carry

    lax.fori_loop(0, 2 * chunks + lag, step, 0)

    for c in range(chunks):
        for i in range(1, n_tw):
            kv_copy(c, i, tw).wait_send()
            q_copy(c, i, tw).wait_send()
            out_copy(c, i, tw).wait_send()
            out_copy(c, i, source(i)).wait_recv()
        out_local(c).wait()

        @pl.when(has_up)
        def _():
            halo_up(c, 0).wait_send()

        @pl.when(has_down)
        def _():
            halo_down(c, 0).wait_send()


def body(sizes, queries, video_kv, text_kv, time_embed, gate_weight, window_extent, tile_valid):
    n_th, n_tw = sizes
    frames, tile_rows, tile_cols, model_width = queries.shape
    per_row = frames * tile_cols
    tokens = tile_rows * per_row
    rows = halo_rows(tile_rows, per_row)
    halo = rows * per_row
    span = tokens + 2 * halo
    own_width = model_width // n_tw
    lanes = 2 * GROUP if own_width % (2 * GROUP) == 0 else own_width
    chunks = own_width // lanes
    wide = min(n_tw, 2 * -(-HALO // tile_cols) + 1)

    flat = lanes % GROUP == 0

    q = queries.transpose(0, 2, 1, 3).reshape(tokens, model_width)
    kv = video_kv.transpose(0, 1, 3, 2, 4).reshape(2, tokens, model_width)
    out_form = (tokens, model_width)
    if not flat:
        q = q.reshape(tokens, n_tw, chunks, lanes).transpose(1, 2, 0, 3)
        kv = kv.reshape(2, tokens, n_tw, chunks, lanes).transpose(2, 3, 0, 1, 4)
        out_form = (n_tw, chunks, tokens, lanes)

    ids = np.arange(tokens)
    q_col, q_row = ids // tile_rows % tile_cols, ids % tile_rows
    q_meta = np.stack([q_row, q_col], axis=1).astype(np.int32)
    h_ids = np.arange(halo)
    h_block, h_row = h_ids // rows, h_ids % rows
    k_row = np.concatenate([h_row - rows, q_row, h_row + tile_rows])
    k_col = np.concatenate([h_block % tile_cols, q_col, h_block % tile_cols])
    band = np.floor_divide(k_row, tile_rows) + 1
    k_meta = np.zeros((8, span), np.int32)
    k_meta[0], k_meta[1] = k_row, band
    k_meta[2], k_meta[3] = k_row - (band - 1) * tile_rows, k_col
    picks = np.concatenate([h_block * tile_rows + h_row, h_block * tile_rows + h_row + tile_rows - rows])
    perm = (picks[:, None] == ids[None, :]).astype(np.float32)
    depth = GROUP if time_embed.shape[0] % GROUP == 0 else time_embed.shape[0]

    hbm = pl.BlockSpec(memory_space=pltpu.HBM)
    others = max(n_tw - 1, 1)
    dma = pltpu.SemaphoreType.DMA
    out = pl.pallas_call(
        functools.partial(kernel, (n_th, n_tw, chunks, lanes, tokens, halo, tile_cols, wide, flat)),
        out_shape=pltpu.VMEM(out_form, jnp.bfloat16),
        in_specs=[hbm] * 10,
        out_specs=hbm,
        scratch_shapes=[
            pltpu.SMEM((2, window_extent.shape[0]), jnp.int32),
            pltpu.SMEM((n_tw, 2, n_th), jnp.int32),
            pltpu.VMEM((time_embed.shape[0] // depth, depth), jnp.bfloat16),
            pltpu.VMEM(q_meta.shape, jnp.int32),
            pltpu.VMEM(k_meta.shape, jnp.int32),
            pltpu.VMEM(perm.shape, jnp.bfloat16),
            pltpu.VMEM((chunks, n_tw, tokens, lanes), jnp.bfloat16),
            pltpu.VMEM((chunks, n_tw, 2, span, lanes), jnp.bfloat16),
            pltpu.VMEM((chunks, n_tw, 2, 2 * halo, lanes), jnp.bfloat16),
            pltpu.VMEM((chunks, n_tw, tokens, lanes), jnp.bfloat16),
            pltpu.VMEM((text_kv.shape[1], 2, text_kv.shape[2]), jnp.bfloat16),
            pltpu.VMEM((chunks, 2, text_kv.shape[1], lanes), jnp.bfloat16),
            pltpu.VMEM(gate_weight.shape, jnp.bfloat16),
            pltpu.VMEM((chunks, 1, lanes), jnp.float32),
            pltpu.VMEM((n_tw, tokens, wide * span), jnp.int32),
            pltpu.VMEM((n_tw, tokens, wide * span), jnp.int32),
            dma((8,)),
            dma((chunks, 3)),
            dma((chunks, others, 2)),
            dma((chunks, others, 2)),
            dma((chunks, 2)),
            dma((chunks, 2)),
            dma((chunks, others)),
            dma((chunks, others)),
        ],
        compiler_params=pltpu.CompilerParams(
            collective_id=0, has_side_effects=True, vmem_limit_bytes=56 * 1024 * 1024
        ),
    )(
        window_extent.T,
        tile_valid.transpose(1, 2, 0),
        q,
        kv,
        text_kv.transpose(1, 0, 2),
        time_embed.reshape(-1, depth),
        gate_weight,
        jnp.asarray(q_meta),
        jnp.asarray(k_meta),
        jnp.asarray(perm, jnp.bfloat16),
    )
    if not flat:
        out = out.transpose(2, 0, 1, 3)
    return out.reshape(frames, tile_cols, tile_rows, model_width).transpose(0, 2, 1, 3)


def solution(mesh):
    placed = (
        P("vid", "th", "tw", None),
        P(None, "vid", "th", "tw", None),
        P(None, "vid", "tw"),
        P("vid"),
        P(None, "tw"),
        P(),
        P("vid", None, None),
    )
    return jax.shard_map(
        functools.partial(body, (mesh.shape["th"], mesh.shape["tw"])),
        mesh=mesh,
        in_specs=placed,
        out_specs=P("vid", "th", "tw", None),
        check_vma=False,
    )
```

```python
import functools

import jax
import jax.numpy as jnp
import numpy as np
from jax import lax
from jax.experimental import pallas as pl
from jax.experimental.pallas import tpu as pltpu
from jax.sharding import PartitionSpec as P

HEAD_DIM = 64
HALO = 3
NEG = -1e30
FAR = 1 << 20
GROUP = 128
MESH = pl.DeviceIdType.MESH


def halo_rows(tile_rows, per_row):
    for rows in range(HALO, tile_rows + 1):
        if rows * per_row % 16 == 0:
            return rows
    return tile_rows


def dot_nt(a, b):
    return lax.dot_general(a, b, (((1,), (1,)), ((), ())), preferred_element_type=jnp.float32)


def kernel(
    dims,
    ext_in,
    valid_in,
    q_in,
    kv_in,
    text_in,
    time_in,
    gw_in,
    qmeta_in,
    kmeta_in,
    perm_in,
    out_ref,
    ext_ref,
    valid_ref,
    time_ref,
    qmeta,
    kmeta,
    perm,
    qbuf,
    kvbuf,
    packed,
    obuf,
    text_raw,
    text_ref,
    gw_ref,
    gate,
    row_gap,
    col_gap,
    pre_sem,
    loc_sem,
    kv_send,
    q_send,
    kv_recv,
    q_recv,
    halo_send,
    halo_recv,
    out_send,
    out_recv,
):
    n_th, n_tw, chunks, lanes, tokens, halo, tile_cols, wide, flat = dims
    span = tokens + 2 * halo
    th = lax.axis_index("th")
    tw = lax.axis_index("tw")
    own = pl.ds(halo, tokens)
    heads_per_chunk = lanes // HEAD_DIM

    def peer(i):
        return lax.rem(tw + i, n_tw)

    def source(i):
        return lax.rem(tw + n_tw - i, n_tw)

    def piece(ref, j, c):
        if flat:
            return ref.at[..., pl.ds(pl.multiple_of((j * chunks + c) * lanes, lanes), lanes)]
        return ref.at[j, c]

    def remote(src, dst, ssem, rsem, where):
        return pltpu.make_async_remote_copy(
            src_ref=src, dst_ref=dst, send_sem=ssem, recv_sem=rsem, device_id=where, device_id_type=MESH
        )

    def kv_copy(c, i, slot):
        return remote(
            piece(kv_in, peer(i), c), kvbuf.at[c, slot, :, own, :], kv_send.at[i - 1], kv_recv.at[c, i - 1], {"tw": peer(i)}
        )

    def q_copy(c, i, slot):
        return remote(
            piece(q_in, peer(i), c), qbuf.at[c, slot], q_send.at[i - 1], q_recv.at[c, i - 1], {"tw": peer(i)}
        )

    def kv_local(c):
        return pltpu.make_async_copy(piece(kv_in, tw, c), kvbuf.at[c, tw, :, own, :], loc_sem.at[0])

    def q_local(c):
        return pltpu.make_async_copy(piece(q_in, tw, c), qbuf.at[c, tw], loc_sem.at[1])

    def halo_up(c, landing):
        dst = pl.ds(halo + tokens, halo)
        return remote(
            packed.at[c, :, :, pl.ds(0, halo), :], kvbuf.at[c, :, :, dst, :], halo_send.at[0], halo_recv.at[c, 0], {"th": th - 1 + landing}
        )

    def halo_down(c, landing):
        dst = pl.ds(0, halo)
        return remote(
            packed.at[c, :, :, pl.ds(halo, halo), :], kvbuf.at[c, :, :, dst, :], halo_send.at[1], halo_recv.at[c, 1], {"th": th + 1 - landing}
        )

    def out_copy(c, i, slot):
        return remote(obuf.at[c, peer(i)], piece(out_ref, slot, c), out_send.at[i - 1], out_recv.at[i - 1], {"tw": peer(i)})

    def out_local(c):
        return pltpu.make_async_copy(obuf.at[c, tw], piece(out_ref, tw, c), loc_sem.at[2])

    has_up = th > 0
    has_down = th < n_th - 1

    barrier = pltpu.get_barrier_semaphore()
    for i in range(1, n_tw):
        pl.semaphore_signal(barrier, inc=1, device_id={"tw": peer(i)}, device_id_type=MESH)

    @pl.when(has_up)
    def _():
        pl.semaphore_signal(barrier, inc=1, device_id={"th": th - 1}, device_id_type=MESH)

    @pl.when(has_down)
    def _():
        pl.semaphore_signal(barrier, inc=1, device_id={"th": th + 1}, device_id_type=MESH)

    pl.semaphore_wait(barrier, n_tw - 1 + has_up.astype(jnp.int32) + has_down.astype(jnp.int32))

    behind = chunks // 2
    for c in range(chunks + behind):
        for i in range(1, n_tw):
            if c < chunks:
                kv_copy(c, i, tw).start()
            if c >= behind:
                q_copy(c - behind, i, tw).start()

    gw_load = pltpu.make_async_copy(gw_in, gw_ref, pre_sem.at[0])
    text_load = pltpu.make_async_copy(text_in, text_raw, pre_sem.at[1])
    for c in range(chunks):
        kv_local(c).start()
        q_local(c).start()
    small = [
        pltpu.make_async_copy(src, dst, pre_sem.at[2])
        for src, dst in (
            [
                (ext_in, ext_ref),
                (valid_in, valid_ref),
                (time_in, time_ref),
                (qmeta_in, qmeta),
                (kmeta_in, kmeta),
                (perm_in, perm),
            ]
        )
    ]
    for load in small:
        load.start()
    gw_load.start()
    text_load.start()

    @pl.when(jnp.logical_not(has_up))
    def _():
        kvbuf[:, :, :, pl.ds(0, halo), :] = jnp.zeros((chunks, n_tw, 2, halo, lanes), kvbuf.dtype)

    @pl.when(jnp.logical_not(has_down))
    def _():
        kvbuf[:, :, :, pl.ds(halo + tokens, halo), :] = jnp.zeros((chunks, n_tw, 2, halo, lanes), kvbuf.dtype)

    def find_gate():
        time = time_ref[...].astype(jnp.float32)
        mod_in = (time / (1.0 + jnp.exp(-time))).astype(jnp.bfloat16)
        gw_load.wait()
        depth = mod_in.shape[1]
        gate_vec = jnp.zeros((1, chunks * lanes), jnp.float32)
        for k in range(mod_in.shape[0]):
            gate_vec = gate_vec + jnp.dot(
                mod_in[k : k + 1], gw_ref[k * depth : (k + 1) * depth], preferred_element_type=jnp.float32
            )
        gate_vec = gate_vec.astype(jnp.bfloat16).astype(jnp.float32)
        for c in range(chunks):
            gate[c] = gate_vec[:, c * lanes : (c + 1) * lanes]

    for load in small:
        load.wait()

    reach = -(-HALO // tile_cols)

    def first_tile(t):
        return jnp.clip(t - reach, 0, n_tw - wide)

    q_row = qmeta[:, 0:1]
    q_col = qmeta[:, 1:2]
    k_row = kmeta[0:1, :]
    k_band = kmeta[1:2, :]
    k_local = kmeta[2:3, :]
    k_col = kmeta[3:4, :]
    above = jnp.maximum(th - 1, 0)
    below = jnp.minimum(th + 1, n_th - 1)

    def distances(t, carry):
        start = first_tile(t)
        for j in range(wide):
            tc = start + j
            limits = []
            for what in range(2):
                up = jnp.where(has_up, valid_ref[tc, what, above], 0)
                mid = valid_ref[tc, what, th]
                down = jnp.where(has_down, valid_ref[tc, what, below], 0)
                limits.append(jnp.where(k_band == 0, up, jnp.where(k_band == 1, mid, down)))
            bad = jnp.where((k_local < limits[0]) & (k_col < limits[1]), 0, FAR)
            row_gap[t, :, pl.ds(j * span, span)] = jnp.abs(k_row - q_row) + bad
            col_gap[t, :, pl.ds(j * span, span)] = jnp.abs(k_col + (tc - t) * tile_cols - q_col)
        return carry

    lax.fori_loop(0, n_tw, distances, 0)
    find_gate()
    text_load.wait()

    def attend(c, t):
        start = first_tile(t)
        q_ok = (q_row < valid_ref[t, 0, th]) & (q_col < valid_ref[t, 1, th])
        rows_apart = row_gap[t]
        cols_apart = col_gap[t]
        for low in range(0, lanes, GROUP):
            width = min(GROUP, lanes - low)
            count = width // HEAD_DIM
            part = pl.ds(low, width)
            q = qbuf[c, t, :, part]
            keys = kvbuf[c, pl.ds(start, wide), 0, :, part].reshape(wide * span, width)
            values = kvbuf[c, pl.ds(start, wide), 1, :, part].reshape(wide * span, width)
            t_keys = text_ref[c, 0, :, part]
            t_values = text_ref[c, 1, :, part]
            lane = lax.broadcasted_iota(jnp.int32, (1, width), 1)
            stacked = []
            for s in range(count):
                mine = (lane >= s * HEAD_DIM) & (lane < (s + 1) * HEAD_DIM)
                stacked.append(q * jnp.where(mine, HEAD_DIM ** -0.5, 0.0).astype(jnp.bfloat16))
            q_all = jnp.concatenate(stacked, axis=0) if count > 1 else stacked[0]
            scores = dot_nt(q_all, keys)
            t_scores = dot_nt(q_all, t_keys)
            weights, t_weights, inverse = [], [], []
            for s in range(count):
                head = tw * (chunks * heads_per_chunk) + c * heads_per_chunk + low // HEAD_DIM + s
                allowed = (rows_apart <= ext_ref[0, head]) & (cols_apart <= ext_ref[1, head])
                sv = jnp.where(allowed, scores[s * tokens : (s + 1) * tokens], NEG)
                st = t_scores[s * tokens : (s + 1) * tokens]
                top = jnp.maximum(jnp.max(sv, axis=-1, keepdims=True), jnp.max(st, axis=-1, keepdims=True))
                ev = jnp.exp(sv - top)
                et = jnp.exp(st - top)
                inverse.append(1.0 / (jnp.sum(ev, axis=-1, keepdims=True) + jnp.sum(et, axis=-1, keepdims=True)))
                weights.append(ev.astype(jnp.bfloat16))
                t_weights.append(et.astype(jnp.bfloat16))
            w_all = jnp.concatenate(weights, axis=0) if count > 1 else weights[0]
            tw_all = jnp.concatenate(t_weights, axis=0) if count > 1 else t_weights[0]
            mixed = jnp.dot(w_all, values, preferred_element_type=jnp.float32) + jnp.dot(
                tw_all, t_values, preferred_element_type=jnp.float32
            )
            result = mixed[0:tokens] * inverse[0]
            for s in range(1, count):
                result = jnp.where(lane >= s * HEAD_DIM, mixed[s * tokens : (s + 1) * tokens] * inverse[s], result)
            result = result * gate[c, :, part]
            obuf[c, t, :, part] = jnp.where(q_ok, result, 0.0).astype(jnp.bfloat16)

    lag = min(2, chunks)
    early = max(0, chunks - 1 - lag)

    def all_of(ref, sem):
        pltpu.make_async_copy(ref, ref, sem).wait()

    def halos_here(c):
        @pl.when(has_down)
        def _():
            halo_up(c, 2).wait_recv()

        @pl.when(has_up)
        def _():
            halo_down(c, 2).wait_recv()

    all_of(kvbuf.at[:, tw, :, own, :], loc_sem.at[0])
    all_of(qbuf.at[:, tw], loc_sem.at[1])

    def step(at, carry):
        @pl.when(at < chunks)
        def _():
            for i in range(1, n_tw):
                kv_copy(at, i, source(i)).wait_recv()

            def pack(j, inner):
                for s in range(2):
                    rows = jnp.dot(perm[...], kvbuf[at, j, s, own, :], preferred_element_type=jnp.float32)
                    packed[at, j, s] = rows.astype(jnp.bfloat16)
                return inner

            lax.fori_loop(0, n_tw, pack, 0)

            @pl.when(has_up)
            def _():
                halo_up(at, 0).start()

            @pl.when(has_down)
            def _():
                halo_down(at, 0).start()

            mine = slice(None) if chunks == 1 else pl.ds(pl.multiple_of(at * lanes, lanes), lanes)
            for s in range(2):
                text_ref[at, s] = text_raw[:, s, mine]

        late = at >= chunks + behind
        own_now = ((at >= lag) & (at < lag + early)) | late
        away_now = (at >= behind) & jnp.logical_not(late)
        own_c = jnp.where(late, at - (chunks + behind) + early, at - lag)
        away_c = at - behind

        def job(i, inner):
            home = i == 0
            c = jnp.where(home, own_c, away_c)

            @pl.when((home & jnp.logical_not(late)) | ((i == 1) & (c >= early)))
            def _():
                halos_here(c)

            @pl.when(jnp.logical_not(home))
            def _():
                q_copy(c, n_tw - i, peer(i)).wait_recv()

            attend(c, peer(i))

            @pl.when(home)
            def _():
                out_local(c).start()

            @pl.when(jnp.logical_not(home))
            def _():
                out_copy(c, i, tw).start()

            return inner

        lax.fori_loop(jnp.where(own_now, 0, 1), jnp.where(away_now, n_tw, 1), job, 0)
        return carry

    lax.fori_loop(0, 2 * chunks + behind - early, step, 0)

    for i in range(1, n_tw):
        all_of(kvbuf.at[:, tw, :, own, :], kv_send.at[i - 1])
        all_of(qbuf.at[:, tw], q_send.at[i - 1])
        all_of(obuf.at[:, tw], out_send.at[i - 1])
    all_of(obuf.at[:, tw], loc_sem.at[2])

    @pl.when(has_up)
    def _():
        all_of(packed.at[:, :, :, pl.ds(0, halo), :], halo_send.at[0])

    @pl.when(has_down)
    def _():
        all_of(packed.at[:, :, :, pl.ds(halo, halo), :], halo_send.at[1])

    for i in range(1, n_tw):
        all_of(obuf.at[:, tw], out_recv.at[i - 1])


def body(sizes, queries, video_kv, text_kv, time_embed, gate_weight, window_extent, tile_valid):
    n_th, n_tw = sizes
    frames, tile_rows, tile_cols, model_width = queries.shape
    per_row = frames * tile_cols
    tokens = tile_rows * per_row
    rows = halo_rows(tile_rows, per_row)
    halo = rows * per_row
    span = tokens + 2 * halo
    own_width = model_width // n_tw
    lanes = 2 * GROUP if own_width % (2 * GROUP) == 0 else own_width
    chunks = own_width // lanes
    wide = min(n_tw, 2 * -(-HALO // tile_cols) + 1)

    flat = lanes % GROUP == 0

    q = queries.transpose(0, 2, 1, 3).reshape(tokens, model_width)
    kv = video_kv.transpose(0, 1, 3, 2, 4).reshape(2, tokens, model_width)
    out_form = (tokens, model_width)
    if not flat:
        q = q.reshape(tokens, n_tw, chunks, lanes).transpose(1, 2, 0, 3)
        kv = kv.reshape(2, tokens, n_tw, chunks, lanes).transpose(2, 3, 0, 1, 4)
        out_form = (n_tw, chunks, tokens, lanes)

    ids = np.arange(tokens)
    q_col, q_row = ids // tile_rows % tile_cols, ids % tile_rows
    q_meta = np.stack([q_row, q_col], axis=1).astype(np.int32)
    h_ids = np.arange(halo)
    h_block, h_row = h_ids // rows, h_ids % rows
    k_row = np.concatenate([h_row - rows, q_row, h_row + tile_rows])
    k_col = np.concatenate([h_block % tile_cols, q_col, h_block % tile_cols])
    band = np.floor_divide(k_row, tile_rows) + 1
    k_meta = np.zeros((8, span), np.int32)
    k_meta[0], k_meta[1] = k_row, band
    k_meta[2], k_meta[3] = k_row - (band - 1) * tile_rows, k_col
    picks = np.concatenate([h_block * tile_rows + h_row, h_block * tile_rows + h_row + tile_rows - rows])
    perm = (picks[:, None] == ids[None, :]).astype(np.float32)
    depth = GROUP if time_embed.shape[0] % GROUP == 0 else time_embed.shape[0]

    hbm = pl.BlockSpec(memory_space=pltpu.HBM)
    others = max(n_tw - 1, 1)
    dma = pltpu.SemaphoreType.DMA
    out = pl.pallas_call(
        functools.partial(kernel, (n_th, n_tw, chunks, lanes, tokens, halo, tile_cols, wide, flat)),
        out_shape=pltpu.VMEM(out_form, jnp.bfloat16),
        in_specs=[hbm] * 10,
        out_specs=hbm,
        scratch_shapes=[
            pltpu.SMEM((2, window_extent.shape[0]), jnp.int32),
            pltpu.SMEM((n_tw, 2, n_th), jnp.int32),
            pltpu.VMEM((time_embed.shape[0] // depth, depth), jnp.bfloat16),
            pltpu.VMEM(q_meta.shape, jnp.int32),
            pltpu.VMEM(k_meta.shape, jnp.int32),
            pltpu.VMEM(perm.shape, jnp.bfloat16),
            pltpu.VMEM((chunks, n_tw, tokens, lanes), jnp.bfloat16),
            pltpu.VMEM((chunks, n_tw, 2, span, lanes), jnp.bfloat16),
            pltpu.VMEM((chunks, n_tw, 2, 2 * halo, lanes), jnp.bfloat16),
            pltpu.VMEM((chunks, n_tw, tokens, lanes), jnp.bfloat16),
            pltpu.VMEM((text_kv.shape[1], 2, text_kv.shape[2]), jnp.bfloat16),
            pltpu.VMEM((chunks, 2, text_kv.shape[1], lanes), jnp.bfloat16),
            pltpu.VMEM(gate_weight.shape, jnp.bfloat16),
            pltpu.VMEM((chunks, 1, lanes), jnp.float32),
            pltpu.VMEM((n_tw, tokens, wide * span), jnp.int32),
            pltpu.VMEM((n_tw, tokens, wide * span), jnp.int32),
            dma((3,)),
            dma((3,)),
            dma((others,)),
            dma((others,)),
            dma((chunks, others)),
            dma((chunks, others)),
            dma((2,)),
            dma((chunks, 2)),
            dma((others,)),
            dma((others,)),
        ],
        compiler_params=pltpu.CompilerParams(
            collective_id=0, has_side_effects=True, vmem_limit_bytes=56 * 1024 * 1024
        ),
    )(
        window_extent.T,
        tile_valid.transpose(1, 2, 0),
        q,
        kv,
        text_kv.transpose(1, 0, 2),
        time_embed.reshape(-1, depth),
        gate_weight,
        jnp.asarray(q_meta),
        jnp.asarray(k_meta),
        jnp.asarray(perm, jnp.bfloat16),
    )
    if not flat:
        out = out.transpose(2, 0, 1, 3)
    return out.reshape(frames, tile_cols, tile_rows, model_width).transpose(0, 2, 1, 3)


def solution(mesh):
    placed = (
        P("vid", "th", "tw", None),
        P(None, "vid", "th", "tw", None),
        P(None, "vid", "tw"),
        P("vid"),
        P(None, "tw"),
        P(),
        P("vid", None, None),
    )
    return jax.shard_map(
        functools.partial(body, (mesh.shape["th"], mesh.shape["tw"])),
        mesh=mesh,
        in_specs=placed,
        out_specs=P("vid", "th", "tw", None),
        check_vma=False,
    )
```

```python
import functools

import jax
import jax.numpy as jnp
import numpy as np
from jax import lax
from jax.experimental import pallas as pl
from jax.experimental.pallas import tpu as pltpu
from jax.sharding import PartitionSpec as P

HEAD_DIM = 64
HALO = 3
NEG = -1e30
FAR = 1 << 20
GROUP = 128
MESH = pl.DeviceIdType.MESH


def halo_rows(tile_rows, per_row):
    for rows in range(HALO, tile_rows + 1):
        if rows * per_row % 16 == 0:
            return rows
    return tile_rows


def dot_nt(a, b):
    return lax.dot_general(a, b, (((1,), (1,)), ((), ())), preferred_element_type=jnp.float32)


def kernel(
    dims,
    ext_in,
    valid_in,
    q_in,
    kv_in,
    text_in,
    time_in,
    gw_in,
    qmeta_in,
    kmeta_in,
    perm_in,
    out_ref,
    ext_ref,
    valid_ref,
    time_ref,
    qmeta,
    kmeta,
    perm,
    qbuf,
    kvbuf,
    packed,
    obuf,
    text_raw,
    text_ref,
    gw_ref,
    gate,
    row_gap,
    col_gap,
    load_sem,
    done_sem,
    kv_recv,
    q_recv,
    halo_recv,
    out_recv,
):
    n_th, n_tw, chunks, lanes, tokens, halo, tile_cols, wide, flat = dims
    span = tokens + 2 * halo
    th = lax.axis_index("th")
    tw = lax.axis_index("tw")
    own = pl.ds(halo, tokens)
    heads_per_chunk = lanes // HEAD_DIM

    def peer(i):
        return lax.rem(tw + i, n_tw)

    def source(i):
        return lax.rem(tw + n_tw - i, n_tw)

    def piece(ref, j, c):
        if flat:
            return ref.at[..., pl.ds(pl.multiple_of((j * chunks + c) * lanes, lanes), lanes)]
        return ref.at[j, c]

    def remote(src, dst, ssem, rsem, where):
        return pltpu.make_async_remote_copy(
            src_ref=src, dst_ref=dst, send_sem=ssem, recv_sem=rsem, device_id=where, device_id_type=MESH
        )

    def kv_copy(c, i, slot):
        return remote(
            piece(kv_in, peer(i), c), kvbuf.at[c, slot, :, own, :], done_sem.at[0], kv_recv.at[c, i - 1], {"tw": peer(i)}
        )

    def q_copy(c, i, slot):
        return remote(
            piece(q_in, peer(i), c), qbuf.at[c, slot], done_sem.at[0], q_recv.at[c, i - 1], {"tw": peer(i)}
        )

    def kv_local(c):
        return pltpu.make_async_copy(piece(kv_in, tw, c), kvbuf.at[c, tw, :, own, :], load_sem.at[1])

    def q_local(c):
        return pltpu.make_async_copy(piece(q_in, tw, c), qbuf.at[c, tw], load_sem.at[1])

    def halo_up(c):
        dst = pl.ds(halo + tokens, halo)
        return remote(
            packed.at[c, :, :, pl.ds(0, halo), :], kvbuf.at[c, :, :, dst, :], done_sem.at[0], halo_recv.at[c], {"th": th - 1}
        )

    def halo_down(c):
        dst = pl.ds(0, halo)
        return remote(
            packed.at[c, :, :, pl.ds(halo, halo), :], kvbuf.at[c, :, :, dst, :], done_sem.at[0], halo_recv.at[c], {"th": th + 1}
        )

    def out_copy(c, i, slot):
        return remote(obuf.at[c, peer(i)], piece(out_ref, slot, c), done_sem.at[0], out_recv.at[i - 1], {"tw": peer(i)})

    def out_local(c):
        return pltpu.make_async_copy(obuf.at[c, tw], piece(out_ref, tw, c), done_sem.at[0])

    has_up = th > 0
    has_down = th < n_th - 1

    barrier = pltpu.get_barrier_semaphore()
    for i in range(1, n_tw):
        pl.semaphore_signal(barrier, inc=1, device_id={"tw": peer(i)}, device_id_type=MESH)

    @pl.when(has_up)
    def _():
        pl.semaphore_signal(barrier, inc=1, device_id={"th": th - 1}, device_id_type=MESH)

    @pl.when(has_down)
    def _():
        pl.semaphore_signal(barrier, inc=1, device_id={"th": th + 1}, device_id_type=MESH)

    pl.semaphore_wait(barrier, n_tw - 1 + has_up.astype(jnp.int32) + has_down.astype(jnp.int32))

    behind = max(chunks - 2, 0)
    for c in range(chunks + behind):
        for i in range(1, n_tw):
            if c < chunks:
                kv_copy(c, i, tw).start()
            if c >= behind:
                q_copy(c - behind, i, tw).start()

    gw_load = pltpu.make_async_copy(gw_in, gw_ref, load_sem.at[0])
    text_load = pltpu.make_async_copy(text_in, text_raw, load_sem.at[1])
    for c in range(chunks):
        kv_local(c).start()
        q_local(c).start()
    small = [
        pltpu.make_async_copy(src, dst, load_sem.at[0])
        for src, dst in (
            [
                (ext_in, ext_ref),
                (valid_in, valid_ref),
                (time_in, time_ref),
                (qmeta_in, qmeta),
                (kmeta_in, kmeta),
                (perm_in, perm),
            ]
        )
    ]
    for load in small:
        load.start()
    gw_load.start()
    text_load.start()

    @pl.when(jnp.logical_not(has_up))
    def _():
        kvbuf[:, :, :, pl.ds(0, halo), :] = jnp.zeros((chunks, n_tw, 2, halo, lanes), kvbuf.dtype)

    @pl.when(jnp.logical_not(has_down))
    def _():
        kvbuf[:, :, :, pl.ds(halo + tokens, halo), :] = jnp.zeros((chunks, n_tw, 2, halo, lanes), kvbuf.dtype)

    def find_gate():
        time = time_ref[...].astype(jnp.float32)
        mod_in = (time / (1.0 + jnp.exp(-time))).astype(jnp.bfloat16)
        depth = mod_in.shape[1]
        gate_vec = jnp.zeros((1, chunks * lanes), jnp.float32)
        for k in range(mod_in.shape[0]):
            gate_vec = gate_vec + jnp.dot(
                mod_in[k : k + 1], gw_ref[k * depth : (k + 1) * depth], preferred_element_type=jnp.float32
            )
        gate_vec = gate_vec.astype(jnp.bfloat16).astype(jnp.float32)
        for c in range(chunks):
            gate[c] = gate_vec[:, c * lanes : (c + 1) * lanes]

    for load in small:
        load.wait()
    gw_load.wait()

    reach = -(-HALO // tile_cols)

    def first_tile(t):
        return jnp.clip(t - reach, 0, n_tw - wide)

    q_row = qmeta[:, 0:1]
    q_col = qmeta[:, 1:2]
    k_row = kmeta[0:1, :]
    k_band = kmeta[1:2, :]
    k_local = kmeta[2:3, :]
    k_col = kmeta[3:4, :]
    above = jnp.maximum(th - 1, 0)
    below = jnp.minimum(th + 1, n_th - 1)

    def distances(t, carry):
        start = first_tile(t)
        for j in range(wide):
            tc = start + j
            limits = []
            for what in range(2):
                up = jnp.where(has_up, valid_ref[tc, what, above], 0)
                mid = valid_ref[tc, what, th]
                down = jnp.where(has_down, valid_ref[tc, what, below], 0)
                limits.append(jnp.where(k_band == 0, up, jnp.where(k_band == 1, mid, down)))
            bad = jnp.where((k_local < limits[0]) & (k_col < limits[1]), 0, FAR)
            row_gap[t, :, pl.ds(j * span, span)] = jnp.abs(k_row - q_row) + bad
            col_gap[t, :, pl.ds(j * span, span)] = jnp.abs(k_col + (tc - t) * tile_cols - q_col)
        return carry

    lax.fori_loop(0, n_tw, distances, 0)
    find_gate()
    text_load.wait()

    def attend(c, t):
        start = first_tile(t)
        q_ok = (q_row < valid_ref[t, 0, th]) & (q_col < valid_ref[t, 1, th])
        rows_apart = row_gap[t]
        cols_apart = col_gap[t]
        for low in range(0, lanes, GROUP):
            width = min(GROUP, lanes - low)
            count = width // HEAD_DIM
            part = pl.ds(low, width)
            q = qbuf[c, t, :, part]
            keys = kvbuf[c, pl.ds(start, wide), 0, :, part].reshape(wide * span, width)
            values = kvbuf[c, pl.ds(start, wide), 1, :, part].reshape(wide * span, width)
            t_keys = text_ref[c, 0, :, part]
            t_values = text_ref[c, 1, :, part]
            lane = lax.broadcasted_iota(jnp.int32, (1, width), 1)
            stacked = []
            for s in range(count):
                mine = (lane >= s * HEAD_DIM) & (lane < (s + 1) * HEAD_DIM)
                stacked.append(q * jnp.where(mine, HEAD_DIM ** -0.5, 0.0).astype(jnp.bfloat16))
            q_all = jnp.concatenate(stacked, axis=0) if count > 1 else stacked[0]
            scores = dot_nt(q_all, keys)
            t_scores = dot_nt(q_all, t_keys)
            weights, t_weights, inverse = [], [], []
            for s in range(count):
                head = tw * (chunks * heads_per_chunk) + c * heads_per_chunk + low // HEAD_DIM + s
                allowed = (rows_apart <= ext_ref[0, head]) & (cols_apart <= ext_ref[1, head])
                sv = jnp.where(allowed, scores[s * tokens : (s + 1) * tokens], NEG)
                st = t_scores[s * tokens : (s + 1) * tokens]
                top = jnp.maximum(jnp.max(sv, axis=-1, keepdims=True), jnp.max(st, axis=-1, keepdims=True))
                ev = jnp.exp(sv - top)
                et = jnp.exp(st - top)
                inverse.append(1.0 / (jnp.sum(ev, axis=-1, keepdims=True) + jnp.sum(et, axis=-1, keepdims=True)))
                weights.append(ev.astype(jnp.bfloat16))
                t_weights.append(et.astype(jnp.bfloat16))
            w_all = jnp.concatenate(weights, axis=0) if count > 1 else weights[0]
            tw_all = jnp.concatenate(t_weights, axis=0) if count > 1 else t_weights[0]
            mixed = jnp.dot(w_all, values, preferred_element_type=jnp.float32) + jnp.dot(
                tw_all, t_values, preferred_element_type=jnp.float32
            )
            result = mixed[0:tokens] * inverse[0]
            for s in range(1, count):
                result = jnp.where(lane >= s * HEAD_DIM, mixed[s * tokens : (s + 1) * tokens] * inverse[s], result)
            result = result * gate[c, :, part]
            obuf[c, t, :, part] = jnp.where(q_ok, result, 0.0).astype(jnp.bfloat16)

    lag = min(2, chunks)
    early = max(0, chunks - 1 - lag)

    def all_of(ref, sem):
        pltpu.make_async_copy(ref, ref, sem).wait()

    def halos_here(c):
        @pl.when(has_down & has_up)
        def _():
            all_of(packed.at[c], halo_recv.at[c])

        @pl.when(has_down != has_up)
        def _():
            all_of(packed.at[c, :, :, pl.ds(0, halo), :], halo_recv.at[c])

    all_of(kvbuf.at[:, tw, :, own, :], load_sem.at[1])
    all_of(qbuf.at[:, tw], load_sem.at[1])

    def step(at, carry):
        @pl.when(at < chunks)
        def _():
            for i in range(1, n_tw):
                kv_copy(at, i, source(i)).wait_recv()

            def pack(j, inner):
                for s in range(2):
                    rows = jnp.dot(perm[...], kvbuf[at, j, s, own, :], preferred_element_type=jnp.float32)
                    packed[at, j, s] = rows.astype(jnp.bfloat16)
                return inner

            lax.fori_loop(0, n_tw, pack, 0)

            @pl.when(has_up)
            def _():
                halo_up(at).start()

            @pl.when(has_down)
            def _():
                halo_down(at).start()

            mine = slice(None) if chunks == 1 else pl.ds(pl.multiple_of(at * lanes, lanes), lanes)
            for s in range(2):
                text_ref[at, s] = text_raw[:, s, mine]

        late = at >= chunks + behind
        own_now = ((at >= lag) & (at < lag + early)) | late
        away_now = (at >= behind) & jnp.logical_not(late)
        own_c = jnp.where(late, at - (chunks + behind) + early, at - lag)
        away_c = at - behind

        def job(i, inner):
            home = i == 0
            c = jnp.where(home, own_c, away_c)

            @pl.when((home & jnp.logical_not(late)) | ((i == 1) & (c >= early)))
            def _():
                halos_here(c)

            @pl.when(jnp.logical_not(home))
            def _():
                q_copy(c, n_tw - i, peer(i)).wait_recv()

            attend(c, peer(i))

            @pl.when(home)
            def _():
                out_local(c).start()

            @pl.when(jnp.logical_not(home))
            def _():
                out_copy(c, i, tw).start()

            return inner

        lax.fori_loop(jnp.where(own_now, 0, 1), jnp.where(away_now, n_tw, 1), job, 0)
        return carry

    lax.fori_loop(0, 2 * chunks + behind - early, step, 0)

    for i in range(1, n_tw):
        all_of(kvbuf.at[:, tw, :, own, :], done_sem.at[0])
        all_of(qbuf.at[:, tw], done_sem.at[0])
        all_of(obuf.at[:, tw], done_sem.at[0])
    all_of(obuf.at[:, tw], done_sem.at[0])

    @pl.when(has_up)
    def _():
        all_of(packed.at[:, :, :, pl.ds(0, halo), :], done_sem.at[0])

    @pl.when(has_down)
    def _():
        all_of(packed.at[:, :, :, pl.ds(halo, halo), :], done_sem.at[0])

    for i in range(1, n_tw):
        all_of(obuf.at[:, tw], out_recv.at[i - 1])


def body(sizes, queries, video_kv, text_kv, time_embed, gate_weight, window_extent, tile_valid):
    n_th, n_tw = sizes
    frames, tile_rows, tile_cols, model_width = queries.shape
    per_row = frames * tile_cols
    tokens = tile_rows * per_row
    rows = halo_rows(tile_rows, per_row)
    halo = rows * per_row
    span = tokens + 2 * halo
    own_width = model_width // n_tw
    lanes = 2 * GROUP if own_width % (2 * GROUP) == 0 else own_width
    chunks = own_width // lanes
    wide = min(n_tw, 2 * -(-HALO // tile_cols) + 1)

    flat = lanes % GROUP == 0

    q = queries.transpose(0, 2, 1, 3).reshape(tokens, model_width)
    kv = video_kv.transpose(0, 1, 3, 2, 4).reshape(2, tokens, model_width)
    out_form = (tokens, model_width)
    if not flat:
        q = q.reshape(tokens, n_tw, chunks, lanes).transpose(1, 2, 0, 3)
        kv = kv.reshape(2, tokens, n_tw, chunks, lanes).transpose(2, 3, 0, 1, 4)
        out_form = (n_tw, chunks, tokens, lanes)

    ids = np.arange(tokens)
    q_col, q_row = ids // tile_rows % tile_cols, ids % tile_rows
    q_meta = np.stack([q_row, q_col], axis=1).astype(np.int32)
    h_ids = np.arange(halo)
    h_block, h_row = h_ids // rows, h_ids % rows
    k_row = np.concatenate([h_row - rows, q_row, h_row + tile_rows])
    k_col = np.concatenate([h_block % tile_cols, q_col, h_block % tile_cols])
    band = np.floor_divide(k_row, tile_rows) + 1
    k_meta = np.zeros((8, span), np.int32)
    k_meta[0], k_meta[1] = k_row, band
    k_meta[2], k_meta[3] = k_row - (band - 1) * tile_rows, k_col
    picks = np.concatenate([h_block * tile_rows + h_row, h_block * tile_rows + h_row + tile_rows - rows])
    perm = (picks[:, None] == ids[None, :]).astype(np.float32)
    depth = GROUP if time_embed.shape[0] % GROUP == 0 else time_embed.shape[0]

    hbm = pl.BlockSpec(memory_space=pltpu.HBM)
    others = max(n_tw - 1, 1)
    dma = pltpu.SemaphoreType.DMA
    out = pl.pallas_call(
        functools.partial(kernel, (n_th, n_tw, chunks, lanes, tokens, halo, tile_cols, wide, flat)),
        out_shape=pltpu.VMEM(out_form, jnp.bfloat16),
        in_specs=[hbm] * 10,
        out_specs=hbm,
        scratch_shapes=[
            pltpu.SMEM((2, window_extent.shape[0]), jnp.int32),
            pltpu.SMEM((n_tw, 2, n_th), jnp.int32),
            pltpu.VMEM((time_embed.shape[0] // depth, depth), jnp.bfloat16),
            pltpu.VMEM(q_meta.shape, jnp.int32),
            pltpu.VMEM(k_meta.shape, jnp.int32),
            pltpu.VMEM(perm.shape, jnp.bfloat16),
            pltpu.VMEM((chunks, n_tw, tokens, lanes), jnp.bfloat16),
            pltpu.VMEM((chunks, n_tw, 2, span, lanes), jnp.bfloat16),
            pltpu.VMEM((chunks, n_tw, 2, 2 * halo, lanes), jnp.bfloat16),
            pltpu.VMEM((chunks, n_tw, tokens, lanes), jnp.bfloat16),
            pltpu.VMEM((text_kv.shape[1], 2, text_kv.shape[2]), jnp.bfloat16),
            pltpu.VMEM((chunks, 2, text_kv.shape[1], lanes), jnp.bfloat16),
            pltpu.VMEM(gate_weight.shape, jnp.bfloat16),
            pltpu.VMEM((chunks, 1, lanes), jnp.float32),
            pltpu.VMEM((n_tw, tokens, wide * span), jnp.int32),
            pltpu.VMEM((n_tw, tokens, wide * span), jnp.int32),
            dma((2,)),
            dma((1,)),
            dma((chunks, others)),
            dma((chunks, others)),
            dma((chunks,)),
            dma((others,)),
        ],
        compiler_params=pltpu.CompilerParams(
            collective_id=0, has_side_effects=True, vmem_limit_bytes=56 * 1024 * 1024
        ),
    )(
        window_extent.T,
        tile_valid.transpose(1, 2, 0),
        q,
        kv,
        text_kv.transpose(1, 0, 2),
        time_embed.reshape(-1, depth),
        gate_weight,
        jnp.asarray(q_meta),
        jnp.asarray(k_meta),
        jnp.asarray(perm, jnp.bfloat16),
    )
    if not flat:
        out = out.transpose(2, 0, 1, 3)
    return out.reshape(frames, tile_cols, tile_rows, model_width).transpose(0, 2, 1, 3)


def solution(mesh):
    placed = (
        P("vid", "th", "tw", None),
        P(None, "vid", "th", "tw", None),
        P(None, "vid", "tw"),
        P("vid"),
        P(None, "tw"),
        P(),
        P("vid", None, None),
    )
    return jax.shard_map(
        functools.partial(body, (mesh.shape["th"], mesh.shape["tw"])),
        mesh=mesh,
        in_specs=placed,
        out_specs=P("vid", "th", "tw", None),
        check_vma=False,
    )
```

```python
import functools

import jax
import jax.numpy as jnp
import numpy as np
from jax import lax
from jax.experimental import pallas as pl
from jax.experimental.pallas import tpu as pltpu
from jax.sharding import PartitionSpec as P

HEAD_DIM = 64
HALO = 3
NEG = -1e30
FAR = 1 << 20
GROUP = 128
MESH = pl.DeviceIdType.MESH


def halo_rows(tile_rows, per_row):
    for rows in range(HALO, tile_rows + 1):
        if rows * per_row % 16 == 0:
            return rows
    return tile_rows


def dot_nt(a, b):
    return lax.dot_general(a, b, (((1,), (1,)), ((), ())), preferred_element_type=jnp.float32)


def kernel(
    dims,
    ext_in,
    valid_in,
    q_in,
    kv_in,
    text_in,
    time_in,
    gw_in,
    qmeta_in,
    kmeta_in,
    perm_in,
    out_ref,
    ext_ref,
    valid_ref,
    time_ref,
    qmeta,
    kmeta,
    perm,
    qbuf,
    kvbuf,
    packed,
    obuf,
    text_raw,
    text_ref,
    gw_ref,
    gate,
    window,
    load_sem,
    done_sem,
    kv_recv,
    q_recv,
    halo_recv,
    out_recv,
    held,
    held_recv,
):
    n_th, n_tw, chunks, lanes, tokens, halo, tile_cols, wide, flat = dims
    span = tokens + 2 * halo
    th = lax.axis_index("th")
    tw = lax.axis_index("tw")
    own = pl.ds(halo, tokens)
    heads_per_chunk = lanes // HEAD_DIM

    def peer(i):
        return lax.rem(tw + i, n_tw)

    def source(i):
        return lax.rem(tw + n_tw - i, n_tw)

    def piece(ref, j, c):
        if flat:
            return ref.at[..., pl.ds(pl.multiple_of((j * chunks + c) * lanes, lanes), lanes)]
        return ref.at[j, c]

    def remote(src, dst, ssem, rsem, where):
        return pltpu.make_async_remote_copy(
            src_ref=src, dst_ref=dst, send_sem=ssem, recv_sem=rsem, device_id=where, device_id_type=MESH
        )

    def kv_copy(c, i, slot):
        return remote(
            piece(kv_in, peer(i), c), kvbuf.at[c, slot, :, own, :], done_sem.at[0], kv_recv.at[c, i - 1], {"tw": peer(i)}
        )

    def q_copy(c, i, slot):
        return remote(
            piece(q_in, peer(i), c), qbuf.at[c, slot], done_sem.at[0], q_recv.at[c, i - 1], {"tw": peer(i)}
        )

    def kv_local(c):
        return pltpu.make_async_copy(piece(kv_in, tw, c), kvbuf.at[c, tw, :, own, :], load_sem.at[1])

    def q_local(c):
        return pltpu.make_async_copy(piece(q_in, tw, c), qbuf.at[c, tw], load_sem.at[1])

    def halo_up(c):
        dst = pl.ds(halo + tokens, halo)
        return remote(
            packed.at[c, :, :, pl.ds(0, halo), :], kvbuf.at[c, :, :, dst, :], done_sem.at[0], halo_recv.at[c], {"th": th - 1}
        )

    def halo_down(c):
        dst = pl.ds(0, halo)
        return remote(
            packed.at[c, :, :, pl.ds(halo, halo), :], kvbuf.at[c, :, :, dst, :], done_sem.at[0], halo_recv.at[c], {"th": th + 1}
        )

    def out_copy(c, i, slot):
        return remote(obuf.at[c, peer(i)], piece(out_ref, slot, c), done_sem.at[0], out_recv.at[i - 1], {"tw": peer(i)})

    def detour_copy():
        return remote(
            piece(q_in, peer(1), astray), held, done_sem.at[0], held_recv.at[0], {"th": turn, "tw": peer(1)}
        )

    def detour_last():
        return remote(held, qbuf.at[astray, peer(1)], done_sem.at[0], q_recv.at[astray, 0], {"th": 0})

    def out_local(c):
        return pltpu.make_async_copy(obuf.at[c, tw], piece(out_ref, tw, c), done_sem.at[0])

    has_up = th > 0
    has_down = th < n_th - 1

    barrier = pltpu.get_barrier_semaphore()
    for i in range(1, n_tw):
        pl.semaphore_signal(barrier, inc=1, device_id={"tw": peer(i)}, device_id_type=MESH)

    @pl.when(has_up)
    def _():
        pl.semaphore_signal(barrier, inc=1, device_id={"th": th - 1}, device_id_type=MESH)

    @pl.when(has_down)
    def _():
        pl.semaphore_signal(barrier, inc=1, device_id={"th": th + 1}, device_id_type=MESH)

    pl.semaphore_wait(barrier, n_tw - 1 + has_up.astype(jnp.int32) + has_down.astype(jnp.int32))

    behind = max(chunks - 2, 0)
    lag = min(2, chunks)
    early = max(0, chunks - 1 - lag)
    detour = n_tw == 2 and n_th >= 4 and early > 2 and chunks > behind + 1
    turn = n_th // 2
    astray = chunks - 1 - behind
    for c in range(chunks + behind):
        for i in range(1, n_tw):
            if c < chunks:
                kv_copy(c, i, tw).start()
            if c >= behind and not (detour and c - behind == astray):
                q_copy(c - behind, i, tw).start()
        if detour and c - behind == astray:

            @pl.when(th != 0)
            def _():
                q_copy(astray, 1, tw).start()


    gw_load = pltpu.make_async_copy(gw_in, gw_ref, load_sem.at[0])
    text_load = pltpu.make_async_copy(text_in, text_raw, load_sem.at[1])
    for c in range(chunks):
        kv_local(c).start()
        q_local(c).start()
    small = [
        pltpu.make_async_copy(src, dst, load_sem.at[0])
        for src, dst in (
            [
                (ext_in, ext_ref),
                (valid_in, valid_ref),
                (time_in, time_ref),
                (qmeta_in, qmeta),
                (kmeta_in, kmeta),
                (perm_in, perm),
            ]
        )
    ]
    for load in small:
        load.start()
    gw_load.start()
    text_load.start()

    @pl.when(jnp.logical_not(has_up))
    def _():
        kvbuf[:, :, :, pl.ds(0, halo), :] = jnp.zeros((chunks, n_tw, 2, halo, lanes), kvbuf.dtype)

    @pl.when(jnp.logical_not(has_down))
    def _():
        kvbuf[:, :, :, pl.ds(halo + tokens, halo), :] = jnp.zeros((chunks, n_tw, 2, halo, lanes), kvbuf.dtype)

    def find_gate():
        time = time_ref[...].astype(jnp.float32)
        mod_in = (time / (1.0 + jnp.exp(-time))).astype(jnp.bfloat16)
        depth = mod_in.shape[1]
        gate_vec = jnp.zeros((1, chunks * lanes), jnp.float32)
        for k in range(mod_in.shape[0]):
            gate_vec = gate_vec + jnp.dot(
                mod_in[k : k + 1], gw_ref[k * depth : (k + 1) * depth], preferred_element_type=jnp.float32
            )
        gate_vec = gate_vec.astype(jnp.bfloat16).astype(jnp.float32)
        for c in range(chunks):
            gate[c] = gate_vec[:, c * lanes : (c + 1) * lanes]

    for load in small:
        load.wait()
    gw_load.wait()

    reach = -(-HALO // tile_cols)

    def first_tile(t):
        return jnp.clip(t - reach, 0, n_tw - wide)

    q_row = qmeta[:, 0:1]
    q_col = qmeta[:, 1:2]
    k_row = kmeta[0:1, :]
    k_band = kmeta[1:2, :]
    k_local = kmeta[2:3, :]
    k_col = kmeta[3:4, :]
    above = jnp.maximum(th - 1, 0)
    below = jnp.minimum(th + 1, n_th - 1)

    def windows(t, carry):
        start = first_tile(t)
        for j in range(wide):
            tc = start + j
            limits = []
            for what in range(2):
                up = jnp.where(has_up, valid_ref[tc, what, above], 0)
                mid = valid_ref[tc, what, th]
                down = jnp.where(has_down, valid_ref[tc, what, below], 0)
                limits.append(jnp.where(k_band == 0, up, jnp.where(k_band == 1, mid, down)))
            bad = jnp.where((k_local < limits[0]) & (k_col < limits[1]), 0, FAR)
            row_gap = jnp.abs(k_row - q_row) + bad
            col_gap = jnp.abs(k_col + (tc - t) * tile_cols - q_col)
            for r in range(HALO):
                near = row_gap <= r + 1
                for k in range(HALO):
                    window[t, r * HALO + k, :, pl.ds(j * span, span)] = jnp.where(near & (col_gap <= k + 1), 0.0, NEG)
        return carry

    lax.fori_loop(0, n_tw, windows, 0)
    find_gate()
    text_load.wait()
    texts = text_raw.shape[0]
    padded = text_ref.shape[2]
    if padded > texts:
        text_ref[:, :, texts // 16 * 16 :, :] = jnp.zeros((chunks, 2, padded - texts // 16 * 16, lanes), text_ref.dtype)

    video = wide * span
    beyond = texts // GROUP * GROUP

    def attend(c, t):
        start = first_tile(t)
        q_ok = (q_row < valid_ref[t, 0, th]) & (q_col < valid_ref[t, 1, th])
        tail = lax.broadcasted_iota(jnp.int32, (1, padded - beyond), 1) + beyond
        tail_bias = jnp.where(tail < texts, 0.0, NEG)
        for low in range(0, lanes, GROUP):
            width = min(GROUP, lanes - low)
            count = width // HEAD_DIM
            part = pl.ds(low, width)
            q = qbuf[c, t, :, part]
            keys, values = [
                jnp.concatenate(
                    [kvbuf[c, pl.ds(start, wide), s, :, part].reshape(video, width), text_ref[c, s, :, part]], axis=0
                )
                for s in range(2)
            ]
            lane = lax.broadcasted_iota(jnp.int32, (1, width), 1)
            stacked = []
            for s in range(count):
                mine = (lane >= s * HEAD_DIM) & (lane < (s + 1) * HEAD_DIM)
                stacked.append(q * jnp.where(mine, HEAD_DIM ** -0.5, 0.0).astype(jnp.bfloat16))
            q_all = jnp.concatenate(stacked, axis=0) if count > 1 else stacked[0]
            scores = dot_nt(q_all, keys)
            weights, inverse = [], []
            for s in range(count):
                head = tw * (chunks * heads_per_chunk) + c * heads_per_chunk + low // HEAD_DIM + s
                reach_at = (jnp.clip(ext_ref[0, head], 1, HALO) - 1) * HALO + jnp.clip(ext_ref[1, head], 1, HALO) - 1
                mine = scores[s * tokens : (s + 1) * tokens]
                pieces = [mine[:, :video] + window[t, reach_at]]
                if beyond:
                    pieces.append(mine[:, video : video + beyond])
                if padded > beyond:
                    pieces.append(mine[:, video + beyond :] + tail_bias)
                near = jnp.concatenate(pieces, axis=1)
                top = jnp.max(near, axis=-1, keepdims=True)
                e = jnp.exp(near - top)
                inverse.append(1.0 / jnp.sum(e, axis=-1, keepdims=True))
                weights.append(e.astype(jnp.bfloat16))
            w_all = jnp.concatenate(weights, axis=0) if count > 1 else weights[0]
            mixed = jnp.dot(w_all, values, preferred_element_type=jnp.float32)
            result = mixed[0:tokens] * inverse[0]
            for s in range(1, count):
                result = jnp.where(lane >= s * HEAD_DIM, mixed[s * tokens : (s + 1) * tokens] * inverse[s], result)
            result = result * gate[c, :, part]
            obuf[c, t, :, part] = jnp.where(q_ok, result, 0.0).astype(jnp.bfloat16)

    def all_of(ref, sem):
        pltpu.make_async_copy(ref, ref, sem).wait()

    def halos_here(c):
        @pl.when(has_down & has_up)
        def _():
            all_of(packed.at[c], halo_recv.at[c])

        @pl.when(has_down != has_up)
        def _():
            all_of(packed.at[c, :, :, pl.ds(0, halo), :], halo_recv.at[c])

    all_of(kvbuf.at[:, tw, :, own, :], load_sem.at[1])
    all_of(qbuf.at[:, tw], load_sem.at[1])

    def step(at, carry):
        if detour:

            @pl.when((th == turn) & (at == lag + early - 1))
            def _():
                all_of(held, held_recv.at[0])
                detour_last().start()

        @pl.when(at < chunks)
        def _():
            for i in range(1, n_tw):
                kv_copy(at, i, source(i)).wait_recv()

            def pack(j, inner):
                for s in range(2):
                    rows = jnp.dot(perm[...], kvbuf[at, j, s, own, :], preferred_element_type=jnp.float32)
                    packed[at, j, s] = rows.astype(jnp.bfloat16)
                return inner

            lax.fori_loop(0, n_tw, pack, 0)

            @pl.when(has_up)
            def _():
                halo_up(at).start()

            @pl.when(has_down)
            def _():
                halo_down(at).start()

        @pl.when((at >= lag) & (at < lag + early))
        def _():
            halos_here(at - lag)

        if detour:

            @pl.when((th == 0) & (at == lag))
            def _():
                detour_copy().start()

        @pl.when(at < -(-chunks // 2))
        def _():
            for k in range(min(2, chunks)):
                c = jnp.minimum(2 * at + k, chunks - 1)
                mine = slice(None) if chunks == 1 else pl.ds(pl.multiple_of(c * lanes, lanes), lanes)
                for s in range(2):
                    text_ref[c, s, :texts] = text_raw[:, s, mine]

        late = at >= chunks + behind
        own_now = ((at >= lag) & (at < lag + early)) | late
        away_now = (at >= behind) & jnp.logical_not(late)
        own_c = jnp.where(late, at - (chunks + behind) + early, at - lag)
        away_c = at - behind

        def job(i, inner):
            home = i == 0
            c = jnp.where(home, own_c, away_c)

            @pl.when((i == 1) & (c >= early))
            def _():
                halos_here(c)

            @pl.when(jnp.logical_not(home))
            def _():
                q_copy(c, n_tw - i, peer(i)).wait_recv()

            attend(c, peer(i))

            @pl.when(home)
            def _():
                out_local(c).start()

            @pl.when(jnp.logical_not(home))
            def _():
                out_copy(c, i, tw).start()

            return inner

        lax.fori_loop(jnp.where(own_now, 0, 1), jnp.where(away_now, n_tw, 1), job, 0)
        return carry

    lax.fori_loop(0, 2 * chunks + behind - early, step, 0)

    for i in range(1, n_tw):
        all_of(kvbuf.at[:, tw, :, own, :], done_sem.at[0])
        all_of(qbuf.at[:, tw], done_sem.at[0])
        all_of(obuf.at[:, tw], done_sem.at[0])
    all_of(obuf.at[:, tw], done_sem.at[0])

    if detour:

        @pl.when(th == turn)
        def _():
            all_of(held, done_sem.at[0])

    @pl.when(has_up)
    def _():
        all_of(packed.at[:, :, :, pl.ds(0, halo), :], done_sem.at[0])

    @pl.when(has_down)
    def _():
        all_of(packed.at[:, :, :, pl.ds(halo, halo), :], done_sem.at[0])

    for i in range(1, n_tw):
        all_of(obuf.at[:, tw], out_recv.at[i - 1])


def body(sizes, queries, video_kv, text_kv, time_embed, gate_weight, window_extent, tile_valid):
    n_th, n_tw = sizes
    frames, tile_rows, tile_cols, model_width = queries.shape
    per_row = frames * tile_cols
    tokens = tile_rows * per_row
    rows = halo_rows(tile_rows, per_row)
    halo = rows * per_row
    span = tokens + 2 * halo
    own_width = model_width // n_tw
    lanes = 2 * GROUP if own_width % (2 * GROUP) == 0 else own_width
    chunks = own_width // lanes
    wide = min(n_tw, 2 * -(-HALO // tile_cols) + 1)

    flat = lanes % GROUP == 0

    q = queries.transpose(0, 2, 1, 3).reshape(tokens, model_width)
    kv = video_kv.transpose(0, 1, 3, 2, 4).reshape(2, tokens, model_width)
    out_form = (tokens, model_width)
    if not flat:
        q = q.reshape(tokens, n_tw, chunks, lanes).transpose(1, 2, 0, 3)
        kv = kv.reshape(2, tokens, n_tw, chunks, lanes).transpose(2, 3, 0, 1, 4)
        out_form = (n_tw, chunks, tokens, lanes)

    ids = np.arange(tokens)
    q_col, q_row = ids // tile_rows % tile_cols, ids % tile_rows
    q_meta = np.stack([q_row, q_col], axis=1).astype(np.int32)
    h_ids = np.arange(halo)
    h_block, h_row = h_ids // rows, h_ids % rows
    k_row = np.concatenate([h_row - rows, q_row, h_row + tile_rows])
    k_col = np.concatenate([h_block % tile_cols, q_col, h_block % tile_cols])
    band = np.floor_divide(k_row, tile_rows) + 1
    k_meta = np.zeros((8, span), np.int32)
    k_meta[0], k_meta[1] = k_row, band
    k_meta[2], k_meta[3] = k_row - (band - 1) * tile_rows, k_col
    picks = np.concatenate([h_block * tile_rows + h_row, h_block * tile_rows + h_row + tile_rows - rows])
    perm = (picks[:, None] == ids[None, :]).astype(np.float32)
    depth = GROUP if time_embed.shape[0] % GROUP == 0 else time_embed.shape[0]

    hbm = pl.BlockSpec(memory_space=pltpu.HBM)
    others = max(n_tw - 1, 1)
    dma = pltpu.SemaphoreType.DMA
    out = pl.pallas_call(
        functools.partial(kernel, (n_th, n_tw, chunks, lanes, tokens, halo, tile_cols, wide, flat)),
        out_shape=pltpu.VMEM(out_form, jnp.bfloat16),
        in_specs=[hbm] * 10,
        out_specs=hbm,
        scratch_shapes=[
            pltpu.SMEM((2, window_extent.shape[0]), jnp.int32),
            pltpu.SMEM((n_tw, 2, n_th), jnp.int32),
            pltpu.VMEM((time_embed.shape[0] // depth, depth), jnp.bfloat16),
            pltpu.VMEM(q_meta.shape, jnp.int32),
            pltpu.VMEM(k_meta.shape, jnp.int32),
            pltpu.VMEM(perm.shape, jnp.bfloat16),
            pltpu.VMEM((chunks, n_tw, tokens, lanes), jnp.bfloat16),
            pltpu.VMEM((chunks, n_tw, 2, span, lanes), jnp.bfloat16),
            pltpu.VMEM((chunks, n_tw, 2, 2 * halo, lanes), jnp.bfloat16),
            pltpu.VMEM((chunks, n_tw, tokens, lanes), jnp.bfloat16),
            pltpu.VMEM((text_kv.shape[1], 2, text_kv.shape[2]), jnp.bfloat16),
            pltpu.VMEM((chunks, 2, -(-text_kv.shape[1] // GROUP) * GROUP, lanes), jnp.bfloat16),
            pltpu.VMEM(gate_weight.shape, jnp.bfloat16),
            pltpu.VMEM((chunks, 1, lanes), jnp.float32),
            pltpu.VMEM((n_tw, HALO * HALO, tokens, wide * span), jnp.float32),
            dma((2,)),
            dma((1,)),
            dma((chunks, others)),
            dma((chunks, others)),
            dma((chunks,)),
            dma((others,)),
            pltpu.VMEM((tokens, lanes), jnp.bfloat16),
            dma((1,)),
        ],
        compiler_params=pltpu.CompilerParams(
            collective_id=0, has_side_effects=True, vmem_limit_bytes=56 * 1024 * 1024
        ),
    )(
        window_extent.T,
        tile_valid.transpose(1, 2, 0),
        q,
        kv,
        text_kv.transpose(1, 0, 2),
        time_embed.reshape(-1, depth),
        gate_weight,
        jnp.asarray(q_meta),
        jnp.asarray(k_meta),
        jnp.asarray(perm, jnp.bfloat16),
    )
    if not flat:
        out = out.transpose(2, 0, 1, 3)
    return out.reshape(frames, tile_cols, tile_rows, model_width).transpose(0, 2, 1, 3)


def solution(mesh):
    placed = (
        P("vid", "th", "tw", None),
        P(None, "vid", "th", "tw", None),
        P(None, "vid", "tw"),
        P("vid"),
        P(None, "tw"),
        P(),
        P("vid", None, None),
    )
    return jax.shard_map(
        functools.partial(body, (mesh.shape["th"], mesh.shape["tw"])),
        mesh=mesh,
        in_specs=placed,
        out_specs=P("vid", "th", "tw", None),
        check_vma=False,
    )
```

```python
import functools

import jax
import jax.numpy as jnp
import numpy as np
from jax import lax
from jax.experimental import pallas as pl
from jax.experimental.pallas import tpu as pltpu
from jax.sharding import PartitionSpec as P

HEAD_DIM = 64
HALO = 3
NEG = -1e30
FAR = 1 << 20
GROUP = 128
MESH = pl.DeviceIdType.MESH


def halo_rows(tile_rows, per_row):
    for rows in range(HALO, tile_rows + 1):
        if rows * per_row % 16 == 0:
            return rows
    return tile_rows


def dot_nt(a, b):
    return lax.dot_general(a, b, (((1,), (1,)), ((), ())), preferred_element_type=jnp.float32)


def kernel(
    dims,
    ext_in,
    valid_in,
    q_in,
    kv_in,
    text_in,
    time_in,
    gw_in,
    qmeta_in,
    kmeta_in,
    perm_in,
    out_ref,
    ext_ref,
    valid_ref,
    time_ref,
    qmeta,
    kmeta,
    perm,
    qbuf,
    kvbuf,
    packed,
    obuf,
    text_raw,
    text_ref,
    gw_ref,
    gate,
    window,
    load_sem,
    done_sem,
    kv_recv,
    q_recv,
    halo_recv,
    out_recv,
    held,
    held_recv,
):
    n_th, n_tw, chunks, lanes, tokens, halo, tile_cols, wide, flat = dims
    span = tokens + 2 * halo
    th = lax.axis_index("th")
    tw = lax.axis_index("tw")
    own = pl.ds(halo, tokens)
    heads_per_chunk = lanes // HEAD_DIM

    def peer(i):
        return lax.rem(tw + i, n_tw)

    def source(i):
        return lax.rem(tw + n_tw - i, n_tw)

    def piece(ref, j, c):
        if flat:
            return ref.at[..., pl.ds(pl.multiple_of((j * chunks + c) * lanes, lanes), lanes)]
        return ref.at[j, c]

    def remote(src, dst, ssem, rsem, where):
        return pltpu.make_async_remote_copy(
            src_ref=src, dst_ref=dst, send_sem=ssem, recv_sem=rsem, device_id=where, device_id_type=MESH
        )

    def kv_copy(c, i, slot):
        return remote(
            piece(kv_in, peer(i), c), kvbuf.at[c, slot, :, own, :], done_sem.at[0], kv_recv.at[c, i - 1], {"tw": peer(i)}
        )

    def q_copy(c, i, slot):
        return remote(
            piece(q_in, peer(i), c), qbuf.at[c, slot], done_sem.at[0], q_recv.at[c, i - 1], {"tw": peer(i)}
        )

    def kv_local(c):
        return pltpu.make_async_copy(piece(kv_in, tw, c), kvbuf.at[c, tw, :, own, :], load_sem.at[1])

    def q_local(c):
        return pltpu.make_async_copy(piece(q_in, tw, c), qbuf.at[c, tw], load_sem.at[1])

    def halo_up(c):
        dst = pl.ds(halo + tokens, halo)
        return remote(
            packed.at[c, :, :, pl.ds(0, halo), :], kvbuf.at[c, :, :, dst, :], done_sem.at[0], halo_recv.at[c], {"th": th - 1}
        )

    def halo_down(c):
        dst = pl.ds(0, halo)
        return remote(
            packed.at[c, :, :, pl.ds(halo, halo), :], kvbuf.at[c, :, :, dst, :], done_sem.at[0], halo_recv.at[c], {"th": th + 1}
        )

    def out_copy(c, i, slot):
        return remote(obuf.at[c, peer(i)], piece(out_ref, slot, c), done_sem.at[0], out_recv.at[i - 1], {"tw": peer(i)})

    def detour_copy():
        return remote(
            piece(q_in, peer(1), astray), held, done_sem.at[0], held_recv.at[0], {"th": turn, "tw": peer(1)}
        )

    def detour_last():
        return remote(held, qbuf.at[astray, peer(1)], done_sem.at[0], q_recv.at[astray, 0], {"th": 0})

    def out_local(c):
        return pltpu.make_async_copy(obuf.at[c, tw], piece(out_ref, tw, c), done_sem.at[0])

    has_up = th > 0
    has_down = th < n_th - 1

    barrier = pltpu.get_barrier_semaphore()
    for i in range(1, n_tw):
        pl.semaphore_signal(barrier, inc=1, device_id={"tw": peer(i)}, device_id_type=MESH)

    @pl.when(has_up)
    def _():
        pl.semaphore_signal(barrier, inc=1, device_id={"th": th - 1}, device_id_type=MESH)

    @pl.when(has_down)
    def _():
        pl.semaphore_signal(barrier, inc=1, device_id={"th": th + 1}, device_id_type=MESH)

    pl.semaphore_wait(barrier, n_tw - 1 + has_up.astype(jnp.int32) + has_down.astype(jnp.int32))

    behind = max(chunks - 2, 0)
    lag = min(2, chunks)
    early = max(0, chunks - 1 - lag)
    detour = n_tw == 2 and n_th >= 4 and early > 2 and chunks > behind + 1
    turn = 2
    astray = chunks - 1 - behind
    for c in range(chunks + behind):
        for i in range(1, n_tw):
            if c < chunks:
                kv_copy(c, i, tw).start()
            if c >= behind and not (detour and c - behind == astray):
                q_copy(c - behind, i, tw).start()
        if detour and c - behind == astray:

            @pl.when(th != 0)
            def _():
                q_copy(astray, 1, tw).start()

    gw_load = pltpu.make_async_copy(gw_in, gw_ref, load_sem.at[0])
    text_load = pltpu.make_async_copy(text_in, text_raw, load_sem.at[1])
    for c in range(chunks):
        kv_local(c).start()
        q_local(c).start()
    small = [
        pltpu.make_async_copy(src, dst, load_sem.at[0])
        for src, dst in (
            [
                (ext_in, ext_ref),
                (valid_in, valid_ref),
                (time_in, time_ref),
                (qmeta_in, qmeta),
                (kmeta_in, kmeta),
                (perm_in, perm),
            ]
        )
    ]
    for load in small:
        load.start()
    gw_load.start()
    text_load.start()

    @pl.when(jnp.logical_not(has_up))
    def _():
        kvbuf[:, :, :, pl.ds(0, halo), :] = jnp.zeros((chunks, n_tw, 2, halo, lanes), kvbuf.dtype)

    @pl.when(jnp.logical_not(has_down))
    def _():
        kvbuf[:, :, :, pl.ds(halo + tokens, halo), :] = jnp.zeros((chunks, n_tw, 2, halo, lanes), kvbuf.dtype)

    def find_gate():
        time = time_ref[...].astype(jnp.float32)
        mod_in = (time / (1.0 + jnp.exp(-time))).astype(jnp.bfloat16)
        depth = mod_in.shape[1]
        gate_vec = jnp.zeros((1, chunks * lanes), jnp.float32)
        for k in range(mod_in.shape[0]):
            gate_vec = gate_vec + jnp.dot(
                mod_in[k : k + 1], gw_ref[k * depth : (k + 1) * depth], preferred_element_type=jnp.float32
            )
        gate_vec = gate_vec.astype(jnp.bfloat16).astype(jnp.float32)
        for c in range(chunks):
            gate[c] = gate_vec[:, c * lanes : (c + 1) * lanes]

    for load in small:
        load.wait()
    gw_load.wait()

    reach = -(-HALO // tile_cols)

    def first_tile(t):
        return jnp.clip(t - reach, 0, n_tw - wide)

    q_row = qmeta[:, 0:1]
    q_col = qmeta[:, 1:2]
    k_row = kmeta[0:1, :]
    k_band = kmeta[1:2, :]
    k_local = kmeta[2:3, :]
    k_col = kmeta[3:4, :]
    above = jnp.maximum(th - 1, 0)
    below = jnp.minimum(th + 1, n_th - 1)

    def windows(t, carry):
        start = first_tile(t)
        for j in range(wide):
            tc = start + j
            limits = []
            for what in range(2):
                up = jnp.where(has_up, valid_ref[tc, what, above], 0)
                mid = valid_ref[tc, what, th]
                down = jnp.where(has_down, valid_ref[tc, what, below], 0)
                limits.append(jnp.where(k_band == 0, up, jnp.where(k_band == 1, mid, down)))
            bad = jnp.where((k_local < limits[0]) & (k_col < limits[1]), 0, FAR)
            row_gap = jnp.abs(k_row - q_row) + bad
            col_gap = jnp.abs(k_col + (tc - t) * tile_cols - q_col)
            for r in range(HALO):
                near = row_gap <= r + 1
                for k in range(HALO):
                    window[t, r * HALO + k, :, pl.ds(j * span, span)] = jnp.where(near & (col_gap <= k + 1), 0.0, NEG)
        return carry

    lax.fori_loop(0, n_tw, windows, 0)
    find_gate()
    text_load.wait()
    texts = text_raw.shape[0]
    padded = text_ref.shape[2]
    if padded > texts:
        text_ref[:, :, texts // 16 * 16 :, :] = jnp.zeros((chunks, 2, padded - texts // 16 * 16, lanes), text_ref.dtype)

    video = wide * span
    beyond = texts // GROUP * GROUP

    def attend(c, t):
        start = first_tile(t)
        q_ok = (q_row < valid_ref[t, 0, th]) & (q_col < valid_ref[t, 1, th])
        tail = lax.broadcasted_iota(jnp.int32, (1, padded - beyond), 1) + beyond
        tail_bias = jnp.where(tail < texts, 0.0, NEG)
        for low in range(0, lanes, GROUP):
            width = min(GROUP, lanes - low)
            count = width // HEAD_DIM
            part = pl.ds(low, width)
            q = qbuf[c, t, :, part]
            keys, values = [
                jnp.concatenate(
                    [kvbuf[c, pl.ds(start, wide), s, :, part].reshape(video, width), text_ref[c, s, :, part]], axis=0
                )
                for s in range(2)
            ]
            lane = lax.broadcasted_iota(jnp.int32, (1, width), 1)
            stacked = []
            for s in range(count):
                mine = (lane >= s * HEAD_DIM) & (lane < (s + 1) * HEAD_DIM)
                stacked.append(q * jnp.where(mine, HEAD_DIM ** -0.5, 0.0).astype(jnp.bfloat16))
            q_all = jnp.concatenate(stacked, axis=0) if count > 1 else stacked[0]
            scores = dot_nt(q_all, keys)
            weights, inverse = [], []
            for s in range(count):
                head = tw * (chunks * heads_per_chunk) + c * heads_per_chunk + low // HEAD_DIM + s
                reach_at = (jnp.clip(ext_ref[0, head], 1, HALO) - 1) * HALO + jnp.clip(ext_ref[1, head], 1, HALO) - 1
                mine = scores[s * tokens : (s + 1) * tokens]
                pieces = [mine[:, :video] + window[t, reach_at]]
                if beyond:
                    pieces.append(mine[:, video : video + beyond])
                if padded > beyond:
                    pieces.append(mine[:, video + beyond :] + tail_bias)
                near = jnp.concatenate(pieces, axis=1)
                top = jnp.max(near, axis=-1, keepdims=True)
                e = jnp.exp(near - top)
                inverse.append(1.0 / jnp.sum(e, axis=-1, keepdims=True))
                weights.append(e.astype(jnp.bfloat16))
            w_all = jnp.concatenate(weights, axis=0) if count > 1 else weights[0]
            mixed = jnp.dot(w_all, values, preferred_element_type=jnp.float32)
            result = mixed[0:tokens] * inverse[0]
            for s in range(1, count):
                result = jnp.where(lane >= s * HEAD_DIM, mixed[s * tokens : (s + 1) * tokens] * inverse[s], result)
            result = result * gate[c, :, part]
            obuf[c, t, :, part] = jnp.where(q_ok, result, 0.0).astype(jnp.bfloat16)

    def all_of(ref, sem):
        pltpu.make_async_copy(ref, ref, sem).wait()

    def halos_here(c):
        @pl.when(has_down & has_up)
        def _():
            all_of(packed.at[c], halo_recv.at[c])

        @pl.when(has_down != has_up)
        def _():
            all_of(packed.at[c, :, :, pl.ds(0, halo), :], halo_recv.at[c])

    all_of(kvbuf.at[:, tw, :, own, :], load_sem.at[1])
    all_of(qbuf.at[:, tw], load_sem.at[1])

    def step(at, carry):
        if detour:

            @pl.when((th == turn) & (at == lag + early - 1))
            def _():
                all_of(held, held_recv.at[0])
                detour_last().start()

        @pl.when(at < chunks)
        def _():
            for i in range(1, n_tw):
                kv_copy(at, i, source(i)).wait_recv()

            def pack(j, inner):
                for s in range(2):
                    rows = jnp.dot(perm[...], kvbuf[at, j, s, own, :], preferred_element_type=jnp.float32)
                    packed[at, j, s] = rows.astype(jnp.bfloat16)
                return inner

            lax.fori_loop(0, n_tw, pack, 0)

            @pl.when(has_up)
            def _():
                halo_up(at).start()

            @pl.when(has_down)
            def _():
                halo_down(at).start()

        @pl.when((at >= lag) & (at < lag + early))
        def _():
            halos_here(at - lag)

        if detour:

            @pl.when((th == 0) & (at == lag))
            def _():
                detour_copy().start()

        @pl.when(at < -(-chunks // 2))
        def _():
            for k in range(min(2, chunks)):
                c = jnp.minimum(2 * at + k, chunks - 1)
                mine = slice(None) if chunks == 1 else pl.ds(pl.multiple_of(c * lanes, lanes), lanes)
                for s in range(2):
                    text_ref[c, s, :texts] = text_raw[:, s, mine]

        late = at >= chunks + behind
        own_now = ((at >= lag) & (at < lag + early)) | late
        away_now = (at >= behind) & jnp.logical_not(late)
        own_c = jnp.where(late, at - (chunks + behind) + early, at - lag)
        away_c = at - behind

        def job(i, inner):
            home = i == 0
            c = jnp.where(home, own_c, away_c)

            @pl.when((i == 1) & (c >= early))
            def _():
                halos_here(c)

            @pl.when(jnp.logical_not(home))
            def _():
                q_copy(c, n_tw - i, peer(i)).wait_recv()

            attend(c, peer(i))

            @pl.when(home)
            def _():
                out_local(c).start()

            @pl.when(jnp.logical_not(home))
            def _():
                out_copy(c, i, tw).start()

            return inner

        lax.fori_loop(jnp.where(own_now, 0, 1), jnp.where(away_now, n_tw, 1), job, 0)
        return carry

    lax.fori_loop(0, 2 * chunks + behind - early, step, 0)

    for i in range(1, n_tw):
        all_of(kvbuf.at[:, tw, :, own, :], done_sem.at[0])
        all_of(qbuf.at[:, tw], done_sem.at[0])
        all_of(obuf.at[:, tw], done_sem.at[0])
    all_of(obuf.at[:, tw], done_sem.at[0])

    if detour:

        @pl.when(th == turn)
        def _():
            all_of(held, done_sem.at[0])

    @pl.when(has_up)
    def _():
        all_of(packed.at[:, :, :, pl.ds(0, halo), :], done_sem.at[0])

    @pl.when(has_down)
    def _():
        all_of(packed.at[:, :, :, pl.ds(halo, halo), :], done_sem.at[0])

    for i in range(1, n_tw):
        all_of(obuf.at[:, tw], out_recv.at[i - 1])


def body(sizes, queries, video_kv, text_kv, time_embed, gate_weight, window_extent, tile_valid):
    n_th, n_tw = sizes
    frames, tile_rows, tile_cols, model_width = queries.shape
    per_row = frames * tile_cols
    tokens = tile_rows * per_row
    rows = halo_rows(tile_rows, per_row)
    halo = rows * per_row
    span = tokens + 2 * halo
    own_width = model_width // n_tw
    lanes = 2 * GROUP if own_width % (2 * GROUP) == 0 else own_width
    chunks = own_width // lanes
    wide = min(n_tw, 2 * -(-HALO // tile_cols) + 1)

    flat = lanes % GROUP == 0

    q = queries.transpose(0, 2, 1, 3).reshape(tokens, model_width)
    kv = video_kv.transpose(0, 1, 3, 2, 4).reshape(2, tokens, model_width)
    out_form = (tokens, model_width)
    if not flat:
        q = q.reshape(tokens, n_tw, chunks, lanes).transpose(1, 2, 0, 3)
        kv = kv.reshape(2, tokens, n_tw, chunks, lanes).transpose(2, 3, 0, 1, 4)
        out_form = (n_tw, chunks, tokens, lanes)

    ids = np.arange(tokens)
    q_col, q_row = ids // tile_rows % tile_cols, ids % tile_rows
    q_meta = np.stack([q_row, q_col], axis=1).astype(np.int32)
    h_ids = np.arange(halo)
    h_block, h_row = h_ids // rows, h_ids % rows
    k_row = np.concatenate([h_row - rows, q_row, h_row + tile_rows])
    k_col = np.concatenate([h_block % tile_cols, q_col, h_block % tile_cols])
    band = np.floor_divide(k_row, tile_rows) + 1
    k_meta = np.zeros((8, span), np.int32)
    k_meta[0], k_meta[1] = k_row, band
    k_meta[2], k_meta[3] = k_row - (band - 1) * tile_rows, k_col
    picks = np.concatenate([h_block * tile_rows + h_row, h_block * tile_rows + h_row + tile_rows - rows])
    perm = (picks[:, None] == ids[None, :]).astype(np.float32)
    depth = GROUP if time_embed.shape[0] % GROUP == 0 else time_embed.shape[0]

    hbm = pl.BlockSpec(memory_space=pltpu.HBM)
    others = max(n_tw - 1, 1)
    dma = pltpu.SemaphoreType.DMA
    out = pl.pallas_call(
        functools.partial(kernel, (n_th, n_tw, chunks, lanes, tokens, halo, tile_cols, wide, flat)),
        out_shape=pltpu.VMEM(out_form, jnp.bfloat16),
        in_specs=[hbm] * 10,
        out_specs=hbm,
        scratch_shapes=[
            pltpu.SMEM((2, window_extent.shape[0]), jnp.int32),
            pltpu.SMEM((n_tw, 2, n_th), jnp.int32),
            pltpu.VMEM((time_embed.shape[0] // depth, depth), jnp.bfloat16),
            pltpu.VMEM(q_meta.shape, jnp.int32),
            pltpu.VMEM(k_meta.shape, jnp.int32),
            pltpu.VMEM(perm.shape, jnp.bfloat16),
            pltpu.VMEM((chunks, n_tw, tokens, lanes), jnp.bfloat16),
            pltpu.VMEM((chunks, n_tw, 2, span, lanes), jnp.bfloat16),
            pltpu.VMEM((chunks, n_tw, 2, 2 * halo, lanes), jnp.bfloat16),
            pltpu.VMEM((chunks, n_tw, tokens, lanes), jnp.bfloat16),
            pltpu.VMEM((text_kv.shape[1], 2, text_kv.shape[2]), jnp.bfloat16),
            pltpu.VMEM((chunks, 2, -(-text_kv.shape[1] // GROUP) * GROUP, lanes), jnp.bfloat16),
            pltpu.VMEM(gate_weight.shape, jnp.bfloat16),
            pltpu.VMEM((chunks, 1, lanes), jnp.float32),
            pltpu.VMEM((n_tw, HALO * HALO, tokens, wide * span), jnp.float32),
            dma((2,)),
            dma((1,)),
            dma((chunks, others)),
            dma((chunks, others)),
            dma((chunks,)),
            dma((others,)),
            pltpu.VMEM((tokens, lanes), jnp.bfloat16),
            dma((1,)),
        ],
        compiler_params=pltpu.CompilerParams(
            collective_id=0, has_side_effects=True, vmem_limit_bytes=56 * 1024 * 1024
        ),
    )(
        window_extent.T,
        tile_valid.transpose(1, 2, 0),
        q,
        kv,
        text_kv.transpose(1, 0, 2),
        time_embed.reshape(-1, depth),
        gate_weight,
        jnp.asarray(q_meta),
        jnp.asarray(k_meta),
        jnp.asarray(perm, jnp.bfloat16),
    )
    if not flat:
        out = out.transpose(2, 0, 1, 3)
    return out.reshape(frames, tile_cols, tile_rows, model_width).transpose(0, 2, 1, 3)


def solution(mesh):
    placed = (
        P("vid", "th", "tw", None),
        P(None, "vid", "th", "tw", None),
        P(None, "vid", "tw"),
        P("vid"),
        P(None, "tw"),
        P(),
        P("vid", None, None),
    )
    return jax.shard_map(
        functools.partial(body, (mesh.shape["th"], mesh.shape["tw"])),
        mesh=mesh,
        in_specs=placed,
        out_specs=P("vid", "th", "tw", None),
        check_vma=False,
    )
```

```python
import functools

import jax
import jax.numpy as jnp
import numpy as np
from jax import lax
from jax.experimental import pallas as pl
from jax.experimental.pallas import tpu as pltpu
from jax.sharding import PartitionSpec as P

HEAD_DIM = 64
HALO = 3
NEG = -1e30
FAR = 1 << 20
GROUP = 128
MESH = pl.DeviceIdType.MESH


def halo_rows(tile_rows, per_row):
    for rows in range(HALO, tile_rows + 1):
        if rows * per_row % 16 == 0:
            return rows
    return tile_rows


def dot_nt(a, b):
    return lax.dot_general(a, b, (((1,), (1,)), ((), ())), preferred_element_type=jnp.float32)


def kernel(
    dims,
    ext_in,
    valid_in,
    q_in,
    kv_in,
    text_in,
    time_in,
    gw_in,
    qmeta_in,
    kmeta_in,
    perm_in,
    out_ref,
    ext_ref,
    valid_ref,
    time_ref,
    qmeta,
    kmeta,
    perm,
    qbuf,
    kvbuf,
    packed,
    obuf,
    text_raw,
    text_ref,
    gw_ref,
    gate,
    window,
    done_sem,
    out_recv,
    held,
):
    n_th, n_tw, chunks, lanes, tokens, halo, tile_cols, wide, flat = dims
    th = lax.axis_index("th")
    tw = lax.axis_index("tw")
    own = pl.ds(halo, tokens)
    has_up = th > 0
    has_down = th < n_th - 1
    others = max(n_tw - 1, 1)
    dma = pltpu.SemaphoreType.DMA

    def all_of(ref, sem):
        pltpu.make_async_copy(ref, ref, sem).wait()

    behind = max(chunks - 2, 0)
    lag = min(2, chunks)
    early = max(0, chunks - 1 - lag)
    detour = n_tw == 2 and n_th >= 4 and early > 2 and chunks > behind + 1
    turn = 2
    astray = chunks - 1 - behind

    def gather_and_attend(load_sem, kv_recv, q_recv, halo_recv, held_recv):
        span = tokens + 2 * halo
        heads_per_chunk = lanes // HEAD_DIM

        def peer(i):
            return lax.rem(tw + i, n_tw)

        def source(i):
            return lax.rem(tw + n_tw - i, n_tw)

        def piece(ref, j, c):
            if flat:
                return ref.at[..., pl.ds(pl.multiple_of((j * chunks + c) * lanes, lanes), lanes)]
            return ref.at[j, c]

        def remote(src, dst, ssem, rsem, where):
            return pltpu.make_async_remote_copy(
                src_ref=src, dst_ref=dst, send_sem=ssem, recv_sem=rsem, device_id=where, device_id_type=MESH
            )

        def kv_copy(c, i, slot):
            return remote(
                piece(kv_in, peer(i), c), kvbuf.at[c, slot, :, own, :], done_sem.at[0], kv_recv.at[c, i - 1], {"tw": peer(i)}
            )

        def q_copy(c, i, slot):
            return remote(
                piece(q_in, peer(i), c), qbuf.at[c, slot], done_sem.at[0], q_recv.at[c, i - 1], {"tw": peer(i)}
            )

        def kv_local(c):
            return pltpu.make_async_copy(piece(kv_in, tw, c), kvbuf.at[c, tw, :, own, :], load_sem.at[1])

        def q_local(c):
            return pltpu.make_async_copy(piece(q_in, tw, c), qbuf.at[c, tw], load_sem.at[1])

        def halo_up(c):
            dst = pl.ds(halo + tokens, halo)
            return remote(
                packed.at[c, :, :, pl.ds(0, halo), :], kvbuf.at[c, :, :, dst, :], done_sem.at[0], halo_recv.at[c], {"th": th - 1}
            )

        def halo_down(c):
            dst = pl.ds(0, halo)
            return remote(
                packed.at[c, :, :, pl.ds(halo, halo), :], kvbuf.at[c, :, :, dst, :], done_sem.at[0], halo_recv.at[c], {"th": th + 1}
            )

        def out_copy(c, i, slot):
            return remote(obuf.at[c, peer(i)], piece(out_ref, slot, c), done_sem.at[0], out_recv.at[i - 1], {"tw": peer(i)})

        def detour_copy():
            return remote(
                piece(q_in, peer(1), astray), held, done_sem.at[0], held_recv.at[0], {"th": turn, "tw": peer(1)}
            )

        def detour_last():
            return remote(held, qbuf.at[astray, peer(1)], done_sem.at[0], q_recv.at[astray, 0], {"th": 0})

        def out_local(c):
            return pltpu.make_async_copy(obuf.at[c, tw], piece(out_ref, tw, c), done_sem.at[0])

        barrier = pltpu.get_barrier_semaphore()
        for i in range(1, n_tw):
            pl.semaphore_signal(barrier, inc=1, device_id={"tw": peer(i)}, device_id_type=MESH)

        @pl.when(has_up)
        def _():
            pl.semaphore_signal(barrier, inc=1, device_id={"th": th - 1}, device_id_type=MESH)

        @pl.when(has_down)
        def _():
            pl.semaphore_signal(barrier, inc=1, device_id={"th": th + 1}, device_id_type=MESH)

        pl.semaphore_wait(barrier, n_tw - 1 + has_up.astype(jnp.int32) + has_down.astype(jnp.int32))

        for c in range(chunks + behind):
            for i in range(1, n_tw):
                if c < chunks:
                    kv_copy(c, i, tw).start()
                if c >= behind and not (detour and c - behind == astray):
                    q_copy(c - behind, i, tw).start()
            if detour and c - behind == astray:

                @pl.when(th != 0)
                def _():
                    q_copy(astray, 1, tw).start()

        gw_load = pltpu.make_async_copy(gw_in, gw_ref, load_sem.at[0])
        text_load = pltpu.make_async_copy(text_in, text_raw, load_sem.at[1])
        for c in range(chunks):
            kv_local(c).start()
            q_local(c).start()
        small = [
            pltpu.make_async_copy(src, dst, load_sem.at[0])
            for src, dst in (
                [
                    (ext_in, ext_ref),
                    (valid_in, valid_ref),
                    (time_in, time_ref),
                    (qmeta_in, qmeta),
                    (kmeta_in, kmeta),
                    (perm_in, perm),
                ]
            )
        ]
        for load in small:
            load.start()
        gw_load.start()
        text_load.start()

        @pl.when(jnp.logical_not(has_up))
        def _():
            kvbuf[:, :, :, pl.ds(0, halo), :] = jnp.zeros((chunks, n_tw, 2, halo, lanes), kvbuf.dtype)

        @pl.when(jnp.logical_not(has_down))
        def _():
            kvbuf[:, :, :, pl.ds(halo + tokens, halo), :] = jnp.zeros((chunks, n_tw, 2, halo, lanes), kvbuf.dtype)

        def find_gate():
            time = time_ref[...].astype(jnp.float32)
            mod_in = (time / (1.0 + jnp.exp(-time))).astype(jnp.bfloat16)
            depth = mod_in.shape[1]
            gate_vec = jnp.zeros((1, chunks * lanes), jnp.float32)
            for k in range(mod_in.shape[0]):
                gate_vec = gate_vec + jnp.dot(
                    mod_in[k : k + 1], gw_ref[k * depth : (k + 1) * depth], preferred_element_type=jnp.float32
                )
            gate_vec = gate_vec.astype(jnp.bfloat16).astype(jnp.float32)
            for c in range(chunks):
                gate[c] = gate_vec[:, c * lanes : (c + 1) * lanes]

        for load in small:
            load.wait()
        gw_load.wait()

        reach = -(-HALO // tile_cols)

        def first_tile(t):
            return jnp.clip(t - reach, 0, n_tw - wide)

        q_row = qmeta[:, 0:1]
        q_col = qmeta[:, 1:2]
        k_row = kmeta[0:1, :]
        k_band = kmeta[1:2, :]
        k_local = kmeta[2:3, :]
        k_col = kmeta[3:4, :]
        above = jnp.maximum(th - 1, 0)
        below = jnp.minimum(th + 1, n_th - 1)

        def windows(t, carry):
            start = first_tile(t)
            for j in range(wide):
                tc = start + j
                limits = []
                for what in range(2):
                    up = jnp.where(has_up, valid_ref[tc, what, above], 0)
                    mid = valid_ref[tc, what, th]
                    down = jnp.where(has_down, valid_ref[tc, what, below], 0)
                    limits.append(jnp.where(k_band == 0, up, jnp.where(k_band == 1, mid, down)))
                bad = jnp.where((k_local < limits[0]) & (k_col < limits[1]), 0, FAR)
                row_gap = jnp.abs(k_row - q_row) + bad
                col_gap = jnp.abs(k_col + (tc - t) * tile_cols - q_col)
                for r in range(HALO):
                    near = row_gap <= r + 1
                    for k in range(HALO):
                        window[t, r * HALO + k, :, pl.ds(j * span, span)] = jnp.where(near & (col_gap <= k + 1), 0.0, NEG)
            return carry

        lax.fori_loop(0, n_tw, windows, 0)
        find_gate()
        text_load.wait()
        texts = text_raw.shape[0]
        padded = text_ref.shape[2]
        if padded > texts:
            text_ref[:, :, texts // 16 * 16 :, :] = jnp.zeros((chunks, 2, padded - texts // 16 * 16, lanes), text_ref.dtype)

        video = wide * span
        beyond = texts // GROUP * GROUP

        def attend(c, t):
            start = first_tile(t)
            q_ok = (q_row < valid_ref[t, 0, th]) & (q_col < valid_ref[t, 1, th])
            tail = lax.broadcasted_iota(jnp.int32, (1, padded - beyond), 1) + beyond
            tail_bias = jnp.where(tail < texts, 0.0, NEG)
            for low in range(0, lanes, GROUP):
                width = min(GROUP, lanes - low)
                count = width // HEAD_DIM
                part = pl.ds(low, width)
                q = qbuf[c, t, :, part]
                keys, values = [
                    jnp.concatenate(
                        [kvbuf[c, pl.ds(start, wide), s, :, part].reshape(video, width), text_ref[c, s, :, part]], axis=0
                    )
                    for s in range(2)
                ]
                lane = lax.broadcasted_iota(jnp.int32, (1, width), 1)
                stacked = []
                for s in range(count):
                    mine = (lane >= s * HEAD_DIM) & (lane < (s + 1) * HEAD_DIM)
                    stacked.append(q * jnp.where(mine, HEAD_DIM ** -0.5, 0.0).astype(jnp.bfloat16))
                q_all = jnp.concatenate(stacked, axis=0) if count > 1 else stacked[0]
                scores = dot_nt(q_all, keys)
                weights, inverse = [], []
                for s in range(count):
                    head = tw * (chunks * heads_per_chunk) + c * heads_per_chunk + low // HEAD_DIM + s
                    reach_at = (jnp.clip(ext_ref[0, head], 1, HALO) - 1) * HALO + jnp.clip(ext_ref[1, head], 1, HALO) - 1
                    mine = scores[s * tokens : (s + 1) * tokens]
                    pieces = [mine[:, :video] + window[t, reach_at]]
                    if beyond:
                        pieces.append(mine[:, video : video + beyond])
                    if padded > beyond:
                        pieces.append(mine[:, video + beyond :] + tail_bias)
                    near = jnp.concatenate(pieces, axis=1)
                    top = jnp.max(near, axis=-1, keepdims=True)
                    e = jnp.exp(near - top)
                    inverse.append(1.0 / jnp.sum(e, axis=-1, keepdims=True))
                    weights.append(e.astype(jnp.bfloat16))
                w_all = jnp.concatenate(weights, axis=0) if count > 1 else weights[0]
                mixed = jnp.dot(w_all, values, preferred_element_type=jnp.float32)
                result = mixed[0:tokens] * inverse[0]
                for s in range(1, count):
                    result = jnp.where(lane >= s * HEAD_DIM, mixed[s * tokens : (s + 1) * tokens] * inverse[s], result)
                result = result * gate[c, :, part]
                obuf[c, t, :, part] = jnp.where(q_ok, result, 0.0).astype(jnp.bfloat16)

        def halos_here(c):
            @pl.when(has_down & has_up)
            def _():
                all_of(packed.at[c], halo_recv.at[c])

            @pl.when(has_down != has_up)
            def _():
                all_of(packed.at[c, :, :, pl.ds(0, halo), :], halo_recv.at[c])

        all_of(kvbuf.at[:, tw, :, own, :], load_sem.at[1])
        all_of(qbuf.at[:, tw], load_sem.at[1])

        def step(at, carry):
            if detour:

                @pl.when((th == turn) & (at == lag + early - 1))
                def _():
                    all_of(held, held_recv.at[0])
                    detour_last().start()

            @pl.when(at < chunks)
            def _():
                for i in range(1, n_tw):
                    kv_copy(at, i, source(i)).wait_recv()

                def pack(j, inner):
                    for s in range(2):
                        rows = jnp.dot(perm[...], kvbuf[at, j, s, own, :], preferred_element_type=jnp.float32)
                        packed[at, j, s] = rows.astype(jnp.bfloat16)
                    return inner

                lax.fori_loop(0, n_tw, pack, 0)

                @pl.when(has_up)
                def _():
                    halo_up(at).start()

                @pl.when(has_down)
                def _():
                    halo_down(at).start()

            @pl.when((at >= lag) & (at < lag + early))
            def _():
                halos_here(at - lag)

            if detour:

                @pl.when((th == 0) & (at == lag))
                def _():
                    detour_copy().start()

            @pl.when(at < -(-chunks // 2))
            def _():
                for k in range(min(2, chunks)):
                    c = jnp.minimum(2 * at + k, chunks - 1)
                    mine = slice(None) if chunks == 1 else pl.ds(pl.multiple_of(c * lanes, lanes), lanes)
                    for s in range(2):
                        text_ref[c, s, :texts] = text_raw[:, s, mine]

            late = at >= chunks + behind
            own_now = ((at >= lag) & (at < lag + early)) | late
            away_now = (at >= behind) & jnp.logical_not(late)
            own_c = jnp.where(late, at - (chunks + behind) + early, at - lag)
            away_c = at - behind

            def job(i, inner):
                home = i == 0
                c = jnp.where(home, own_c, away_c)

                @pl.when((i == 1) & (c >= early))
                def _():
                    halos_here(c)

                @pl.when(jnp.logical_not(home))
                def _():
                    q_copy(c, n_tw - i, peer(i)).wait_recv()

                attend(c, peer(i))

                @pl.when(home)
                def _():
                    out_local(c).start()

                @pl.when(jnp.logical_not(home))
                def _():
                    out_copy(c, i, tw).start()

                return inner

            lax.fori_loop(jnp.where(own_now, 0, 1), jnp.where(away_now, n_tw, 1), job, 0)
            return carry

        lax.fori_loop(0, 2 * chunks + behind - early, step, 0)

    pl.run_scoped(
        gather_and_attend,
        dma((2,)),
        dma((chunks, others)),
        dma((chunks, others)),
        dma((chunks,)),
        dma((1,)),
    )

    for i in range(1, n_tw):
        all_of(kvbuf.at[:, tw, :, own, :], done_sem.at[0])
        all_of(qbuf.at[:, tw], done_sem.at[0])
        all_of(obuf.at[:, tw], done_sem.at[0])
    all_of(obuf.at[:, tw], done_sem.at[0])

    if detour:

        @pl.when(th == turn)
        def _():
            all_of(held, done_sem.at[0])

    @pl.when(has_up)
    def _():
        all_of(packed.at[:, :, :, pl.ds(0, halo), :], done_sem.at[0])

    @pl.when(has_down)
    def _():
        all_of(packed.at[:, :, :, pl.ds(halo, halo), :], done_sem.at[0])

    for i in range(1, n_tw):
        all_of(obuf.at[:, tw], out_recv.at[i - 1])


def body(sizes, queries, video_kv, text_kv, time_embed, gate_weight, window_extent, tile_valid):
    n_th, n_tw = sizes
    frames, tile_rows, tile_cols, model_width = queries.shape
    per_row = frames * tile_cols
    tokens = tile_rows * per_row
    rows = halo_rows(tile_rows, per_row)
    halo = rows * per_row
    span = tokens + 2 * halo
    own_width = model_width // n_tw
    lanes = 2 * GROUP if own_width % (2 * GROUP) == 0 else own_width
    chunks = own_width // lanes
    wide = min(n_tw, 2 * -(-HALO // tile_cols) + 1)

    flat = lanes % GROUP == 0

    q = queries.transpose(0, 2, 1, 3).reshape(tokens, model_width)
    kv = video_kv.transpose(0, 1, 3, 2, 4).reshape(2, tokens, model_width)
    out_form = (tokens, model_width)
    if not flat:
        q = q.reshape(tokens, n_tw, chunks, lanes).transpose(1, 2, 0, 3)
        kv = kv.reshape(2, tokens, n_tw, chunks, lanes).transpose(2, 3, 0, 1, 4)
        out_form = (n_tw, chunks, tokens, lanes)

    ids = np.arange(tokens)
    q_col, q_row = ids // tile_rows % tile_cols, ids % tile_rows
    q_meta = np.stack([q_row, q_col], axis=1).astype(np.int32)
    h_ids = np.arange(halo)
    h_block, h_row = h_ids // rows, h_ids % rows
    k_row = np.concatenate([h_row - rows, q_row, h_row + tile_rows])
    k_col = np.concatenate([h_block % tile_cols, q_col, h_block % tile_cols])
    band = np.floor_divide(k_row, tile_rows) + 1
    k_meta = np.zeros((8, span), np.int32)
    k_meta[0], k_meta[1] = k_row, band
    k_meta[2], k_meta[3] = k_row - (band - 1) * tile_rows, k_col
    picks = np.concatenate([h_block * tile_rows + h_row, h_block * tile_rows + h_row + tile_rows - rows])
    perm = (picks[:, None] == ids[None, :]).astype(np.float32)
    depth = GROUP if time_embed.shape[0] % GROUP == 0 else time_embed.shape[0]

    hbm = pl.BlockSpec(memory_space=pltpu.HBM)
    others = max(n_tw - 1, 1)
    dma = pltpu.SemaphoreType.DMA
    out = pl.pallas_call(
        functools.partial(kernel, (n_th, n_tw, chunks, lanes, tokens, halo, tile_cols, wide, flat)),
        out_shape=pltpu.VMEM(out_form, jnp.bfloat16),
        in_specs=[hbm] * 10,
        out_specs=hbm,
        scratch_shapes=[
            pltpu.SMEM((2, window_extent.shape[0]), jnp.int32),
            pltpu.SMEM((n_tw, 2, n_th), jnp.int32),
            pltpu.VMEM((time_embed.shape[0] // depth, depth), jnp.bfloat16),
            pltpu.VMEM(q_meta.shape, jnp.int32),
            pltpu.VMEM(k_meta.shape, jnp.int32),
            pltpu.VMEM(perm.shape, jnp.bfloat16),
            pltpu.VMEM((chunks, n_tw, tokens, lanes), jnp.bfloat16),
            pltpu.VMEM((chunks, n_tw, 2, span, lanes), jnp.bfloat16),
            pltpu.VMEM((chunks, n_tw, 2, 2 * halo, lanes), jnp.bfloat16),
            pltpu.VMEM((chunks, n_tw, tokens, lanes), jnp.bfloat16),
            pltpu.VMEM((text_kv.shape[1], 2, text_kv.shape[2]), jnp.bfloat16),
            pltpu.VMEM((chunks, 2, -(-text_kv.shape[1] // GROUP) * GROUP, lanes), jnp.bfloat16),
            pltpu.VMEM(gate_weight.shape, jnp.bfloat16),
            pltpu.VMEM((chunks, 1, lanes), jnp.float32),
            pltpu.VMEM((n_tw, HALO * HALO, tokens, wide * span), jnp.float32),
            dma((1,)),
            dma((others,)),
            pltpu.VMEM((tokens, lanes), jnp.bfloat16),
        ],
        compiler_params=pltpu.CompilerParams(
            collective_id=0, has_side_effects=True, vmem_limit_bytes=56 * 1024 * 1024
        ),
    )(
        window_extent.T,
        tile_valid.transpose(1, 2, 0),
        q,
        kv,
        text_kv.transpose(1, 0, 2),
        time_embed.reshape(-1, depth),
        gate_weight,
        jnp.asarray(q_meta),
        jnp.asarray(k_meta),
        jnp.asarray(perm, jnp.bfloat16),
    )
    if not flat:
        out = out.transpose(2, 0, 1, 3)
    return out.reshape(frames, tile_cols, tile_rows, model_width).transpose(0, 2, 1, 3)


def solution(mesh):
    placed = (
        P("vid", "th", "tw", None),
        P(None, "vid", "th", "tw", None),
        P(None, "vid", "tw"),
        P("vid"),
        P(None, "tw"),
        P(),
        P("vid", None, None),
    )
    return jax.shard_map(
        functools.partial(body, (mesh.shape["th"], mesh.shape["tw"])),
        mesh=mesh,
        in_specs=placed,
        out_specs=P("vid", "th", "tw", None),
        check_vma=False,
    )
```

```python
import functools

import jax
import jax.numpy as jnp
import numpy as np
from jax import lax
from jax.experimental import pallas as pl
from jax.experimental.pallas import tpu as pltpu
from jax.sharding import PartitionSpec as P

HEAD_DIM = 64
HALO = 3
NEG = -1e30
FAR = 1 << 20
GROUP = 128
MESH = pl.DeviceIdType.MESH


def halo_rows(tile_rows, per_row):
    for rows in range(HALO, tile_rows + 1):
        if rows * per_row % 16 == 0:
            return rows
    return tile_rows


def dot_nt(a, b):
    return lax.dot_general(a, b, (((1,), (1,)), ((), ())), preferred_element_type=jnp.float32)


def kernel(
    dims,
    ext_in,
    valid_in,
    q_in,
    kv_in,
    text_in,
    time_in,
    gw_in,
    qmeta_in,
    kmeta_in,
    perm_in,
    out_ref,
    ext_ref,
    valid_ref,
    time_ref,
    qmeta,
    kmeta,
    perm,
    qbuf,
    kvbuf,
    packed,
    obuf,
    text_raw,
    text_ref,
    gw_ref,
    gate,
    window,
    done_sem,
    out_recv,
    held,
):
    n_th, n_tw, chunks, lanes, tokens, halo, tile_cols, wide, flat = dims
    th = lax.axis_index("th")
    tw = lax.axis_index("tw")
    own = pl.ds(halo, tokens)
    has_up = th > 0
    has_down = th < n_th - 1
    others = max(n_tw - 1, 1)
    dma = pltpu.SemaphoreType.DMA

    def all_of(ref, sem):
        pltpu.make_async_copy(ref, ref, sem).wait()

    behind = max(chunks - 2, 0)
    lag = min(2, chunks)
    early = max(0, chunks - 1 - lag)
    detour = n_tw == 2 and n_th >= 4 and early > 2 and chunks > behind + 1
    turn = 2
    astray = chunks - 1 - behind

    def gather_and_attend(load_sem, kv_recv, q_recv, halo_recv, held_recv):
        span = tokens + 2 * halo
        heads_per_chunk = lanes // HEAD_DIM

        def peer(i):
            return lax.rem(tw + i, n_tw)

        def source(i):
            return lax.rem(tw + n_tw - i, n_tw)

        def piece(ref, j, c):
            if flat:
                return ref.at[..., pl.ds(pl.multiple_of((j * chunks + c) * lanes, lanes), lanes)]
            return ref.at[j, c]

        def remote(src, dst, ssem, rsem, where):
            return pltpu.make_async_remote_copy(
                src_ref=src, dst_ref=dst, send_sem=ssem, recv_sem=rsem, device_id=where, device_id_type=MESH
            )

        def kv_copy(c, i, slot):
            return remote(
                piece(kv_in, peer(i), c), kvbuf.at[c, slot, :, own, :], done_sem.at[0], kv_recv.at[c, i - 1], {"tw": peer(i)}
            )

        def q_copy(c, i, slot):
            return remote(
                piece(q_in, peer(i), c), qbuf.at[c, slot], done_sem.at[0], q_recv.at[c, i - 1], {"tw": peer(i)}
            )

        def kv_local(c):
            return pltpu.make_async_copy(piece(kv_in, tw, c), kvbuf.at[c, tw, :, own, :], load_sem.at[1])

        def q_local(c):
            return pltpu.make_async_copy(piece(q_in, tw, c), qbuf.at[c, tw], load_sem.at[1])

        def halo_up(c):
            dst = pl.ds(halo + tokens, halo)
            return remote(
                packed.at[c, :, :, pl.ds(0, halo), :], kvbuf.at[c, :, :, dst, :], done_sem.at[0], halo_recv.at[c], {"th": th - 1}
            )

        def halo_down(c):
            dst = pl.ds(0, halo)
            return remote(
                packed.at[c, :, :, pl.ds(halo, halo), :], kvbuf.at[c, :, :, dst, :], done_sem.at[0], halo_recv.at[c], {"th": th + 1}
            )

        def out_copy(c, i, slot):
            return remote(obuf.at[c, peer(i)], piece(out_ref, slot, c), done_sem.at[0], out_recv.at[i - 1], {"tw": peer(i)})

        def detour_copy():
            return remote(
                piece(q_in, peer(1), astray), held, done_sem.at[0], held_recv.at[0], {"th": turn, "tw": peer(1)}
            )

        def detour_last():
            return remote(held, qbuf.at[astray, peer(1)], done_sem.at[0], q_recv.at[astray, 0], {"th": 0})

        def out_local(c):
            return pltpu.make_async_copy(obuf.at[c, tw], piece(out_ref, tw, c), done_sem.at[0])

        barrier = pltpu.get_barrier_semaphore()
        for i in range(1, n_tw):
            pl.semaphore_signal(barrier, inc=1, device_id={"tw": peer(i)}, device_id_type=MESH)

        @pl.when(has_up)
        def _():
            pl.semaphore_signal(barrier, inc=1, device_id={"th": th - 1}, device_id_type=MESH)

        @pl.when(has_down)
        def _():
            pl.semaphore_signal(barrier, inc=1, device_id={"th": th + 1}, device_id_type=MESH)

        gw_load = pltpu.make_async_copy(gw_in, gw_ref, load_sem.at[0])
        text_load = pltpu.make_async_copy(text_in, text_raw, load_sem.at[1])
        for c in range(chunks):
            kv_local(c).start()
            q_local(c).start()
        small = [
            pltpu.make_async_copy(src, dst, load_sem.at[0])
            for src, dst in (
                [
                    (ext_in, ext_ref),
                    (valid_in, valid_ref),
                    (time_in, time_ref),
                    (qmeta_in, qmeta),
                    (kmeta_in, kmeta),
                    (perm_in, perm),
                ]
            )
        ]
        for load in small:
            load.start()
        gw_load.start()
        text_load.start()

        pl.semaphore_wait(barrier, n_tw - 1 + has_up.astype(jnp.int32) + has_down.astype(jnp.int32))

        for c in range(chunks + behind):
            for i in range(1, n_tw):
                if c < chunks:
                    kv_copy(c, i, tw).start()
                if c >= behind and not (detour and c - behind == astray):
                    q_copy(c - behind, i, tw).start()
            if detour and c - behind == astray:

                @pl.when(th != 0)
                def _():
                    q_copy(astray, 1, tw).start()

        @pl.when(jnp.logical_not(has_up))
        def _():
            kvbuf[:, :, :, pl.ds(0, halo), :] = jnp.zeros((chunks, n_tw, 2, halo, lanes), kvbuf.dtype)

        @pl.when(jnp.logical_not(has_down))
        def _():
            kvbuf[:, :, :, pl.ds(halo + tokens, halo), :] = jnp.zeros((chunks, n_tw, 2, halo, lanes), kvbuf.dtype)

        def find_gate():
            time = time_ref[...].astype(jnp.float32)
            mod_in = (time / (1.0 + jnp.exp(-time))).astype(jnp.bfloat16)
            depth = mod_in.shape[1]
            gate_vec = jnp.zeros((1, chunks * lanes), jnp.float32)
            for k in range(mod_in.shape[0]):
                gate_vec = gate_vec + jnp.dot(
                    mod_in[k : k + 1], gw_ref[k * depth : (k + 1) * depth], preferred_element_type=jnp.float32
                )
            gate_vec = gate_vec.astype(jnp.bfloat16).astype(jnp.float32)
            for c in range(chunks):
                gate[c] = gate_vec[:, c * lanes : (c + 1) * lanes]

        for load in small:
            load.wait()
        gw_load.wait()

        reach = -(-HALO // tile_cols)

        def first_tile(t):
            return jnp.clip(t - reach, 0, n_tw - wide)

        q_row = qmeta[:, 0:1]
        q_col = qmeta[:, 1:2]
        k_row = kmeta[0:1, :]
        k_band = kmeta[1:2, :]
        k_local = kmeta[2:3, :]
        k_col = kmeta[3:4, :]
        above = jnp.maximum(th - 1, 0)
        below = jnp.minimum(th + 1, n_th - 1)

        def windows(t, carry):
            start = first_tile(t)
            for j in range(wide):
                tc = start + j
                limits = []
                for what in range(2):
                    up = jnp.where(has_up, valid_ref[tc, what, above], 0)
                    mid = valid_ref[tc, what, th]
                    down = jnp.where(has_down, valid_ref[tc, what, below], 0)
                    limits.append(jnp.where(k_band == 0, up, jnp.where(k_band == 1, mid, down)))
                bad = jnp.where((k_local < limits[0]) & (k_col < limits[1]), 0, FAR)
                row_gap = jnp.abs(k_row - q_row) + bad
                col_gap = jnp.abs(k_col + (tc - t) * tile_cols - q_col)
                for r in range(HALO):
                    near = row_gap <= r + 1
                    for k in range(HALO):
                        window[t, r * HALO + k, :, pl.ds(j * span, span)] = jnp.where(near & (col_gap <= k + 1), 0.0, NEG)
            return carry

        lax.fori_loop(0, n_tw, windows, 0)
        find_gate()
        text_load.wait()
        texts = text_raw.shape[0]
        padded = text_ref.shape[2]
        if padded > texts:
            text_ref[:, :, texts // 16 * 16 :, :] = jnp.zeros((chunks, 2, padded - texts // 16 * 16, lanes), text_ref.dtype)

        video = wide * span
        beyond = texts // GROUP * GROUP

        def attend(c, t):
            start = first_tile(t)
            q_ok = (q_row < valid_ref[t, 0, th]) & (q_col < valid_ref[t, 1, th])
            tail = lax.broadcasted_iota(jnp.int32, (1, padded - beyond), 1) + beyond
            tail_bias = jnp.where(tail < texts, 0.0, NEG)
            for low in range(0, lanes, GROUP):
                width = min(GROUP, lanes - low)
                count = width // HEAD_DIM
                part = pl.ds(low, width)
                q = qbuf[c, t, :, part]
                keys, values = [
                    jnp.concatenate(
                        [kvbuf[c, pl.ds(start, wide), s, :, part].reshape(video, width), text_ref[c, s, :, part]], axis=0
                    )
                    for s in range(2)
                ]
                lane = lax.broadcasted_iota(jnp.int32, (1, width), 1)
                stacked = []
                for s in range(count):
                    mine = (lane >= s * HEAD_DIM) & (lane < (s + 1) * HEAD_DIM)
                    stacked.append(q * jnp.where(mine, HEAD_DIM ** -0.5, 0.0).astype(jnp.bfloat16))
                q_all = jnp.concatenate(stacked, axis=0) if count > 1 else stacked[0]
                scores = dot_nt(q_all, keys)
                weights, inverse = [], []
                for s in range(count):
                    head = tw * (chunks * heads_per_chunk) + c * heads_per_chunk + low // HEAD_DIM + s
                    reach_at = (jnp.clip(ext_ref[0, head], 1, HALO) - 1) * HALO + jnp.clip(ext_ref[1, head], 1, HALO) - 1
                    mine = scores[s * tokens : (s + 1) * tokens]
                    pieces = [mine[:, :video] + window[t, reach_at]]
                    if beyond:
                        pieces.append(mine[:, video : video + beyond])
                    if padded > beyond:
                        pieces.append(mine[:, video + beyond :] + tail_bias)
                    near = jnp.concatenate(pieces, axis=1)
                    top = jnp.max(near, axis=-1, keepdims=True)
                    e = jnp.exp(near - top)
                    inverse.append(1.0 / jnp.sum(e, axis=-1, keepdims=True))
                    weights.append(e.astype(jnp.bfloat16))
                w_all = jnp.concatenate(weights, axis=0) if count > 1 else weights[0]
                mixed = jnp.dot(w_all, values, preferred_element_type=jnp.float32)
                result = mixed[0:tokens] * inverse[0]
                for s in range(1, count):
                    result = jnp.where(lane >= s * HEAD_DIM, mixed[s * tokens : (s + 1) * tokens] * inverse[s], result)
                result = result * gate[c, :, part]
                obuf[c, t, :, part] = jnp.where(q_ok, result, 0.0).astype(jnp.bfloat16)

        def halos_here(c):
            @pl.when(has_down & has_up)
            def _():
                all_of(packed.at[c], halo_recv.at[c])

            @pl.when(has_down != has_up)
            def _():
                all_of(packed.at[c, :, :, pl.ds(0, halo), :], halo_recv.at[c])

        all_of(kvbuf.at[:, tw, :, own, :], load_sem.at[1])
        all_of(qbuf.at[:, tw], load_sem.at[1])

        def step(at, carry):
            if detour:

                @pl.when((th == turn) & (at == lag + early - 1))
                def _():
                    all_of(held, held_recv.at[0])
                    detour_last().start()

            @pl.when(at < chunks)
            def _():
                for i in range(1, n_tw):
                    kv_copy(at, i, source(i)).wait_recv()

                def pack(j, inner):
                    for s in range(2):
                        rows = jnp.dot(perm[...], kvbuf[at, j, s, own, :], preferred_element_type=jnp.float32)
                        packed[at, j, s] = rows.astype(jnp.bfloat16)
                    return inner

                lax.fori_loop(0, n_tw, pack, 0)

                @pl.when(has_up)
                def _():
                    halo_up(at).start()

                @pl.when(has_down)
                def _():
                    halo_down(at).start()

            @pl.when((at >= lag) & (at < lag + early))
            def _():
                halos_here(at - lag)

            if detour:

                @pl.when((th == 0) & (at == lag))
                def _():
                    detour_copy().start()

            @pl.when(at < -(-chunks // 2))
            def _():
                for k in range(min(2, chunks)):
                    c = jnp.minimum(2 * at + k, chunks - 1)
                    mine = slice(None) if chunks == 1 else pl.ds(pl.multiple_of(c * lanes, lanes), lanes)
                    for s in range(2):
                        text_ref[c, s, :texts] = text_raw[:, s, mine]

            late = at >= chunks + behind
            own_now = ((at >= lag) & (at < lag + early)) | late
            away_now = (at >= behind) & jnp.logical_not(late)
            own_c = jnp.where(late, at - (chunks + behind) + early, at - lag)
            away_c = at - behind

            def job(i, inner):
                home = i == 0
                c = jnp.where(home, own_c, away_c)

                @pl.when((i == 1) & (c >= early))
                def _():
                    halos_here(c)

                @pl.when(jnp.logical_not(home))
                def _():
                    q_copy(c, n_tw - i, peer(i)).wait_recv()

                attend(c, peer(i))

                @pl.when(home)
                def _():
                    out_local(c).start()

                @pl.when(jnp.logical_not(home))
                def _():
                    out_copy(c, i, tw).start()

                return inner

            lax.fori_loop(jnp.where(own_now, 0, 1), jnp.where(away_now, n_tw, 1), job, 0)
            return carry

        lax.fori_loop(0, 2 * chunks + behind - early, step, 0)

    pl.run_scoped(
        gather_and_attend,
        dma((2,)),
        dma((chunks, others)),
        dma((chunks, others)),
        dma((chunks,)),
        dma((1,)),
    )

    for i in range(1, n_tw):
        all_of(kvbuf.at[:, tw, :, own, :], done_sem.at[0])
        all_of(qbuf.at[:, tw], done_sem.at[0])
        all_of(obuf.at[:, tw], done_sem.at[0])
    all_of(obuf.at[:, tw], done_sem.at[0])

    if detour:

        @pl.when(th == turn)
        def _():
            all_of(held, done_sem.at[0])

    @pl.when(has_up)
    def _():
        all_of(packed.at[:, :, :, pl.ds(0, halo), :], done_sem.at[0])

    @pl.when(has_down)
    def _():
        all_of(packed.at[:, :, :, pl.ds(halo, halo), :], done_sem.at[0])

    for i in range(1, n_tw):
        all_of(obuf.at[:, tw], out_recv.at[i - 1])


def body(sizes, queries, video_kv, text_kv, time_embed, gate_weight, window_extent, tile_valid):
    n_th, n_tw = sizes
    frames, tile_rows, tile_cols, model_width = queries.shape
    per_row = frames * tile_cols
    tokens = tile_rows * per_row
    rows = halo_rows(tile_rows, per_row)
    halo = rows * per_row
    span = tokens + 2 * halo
    own_width = model_width // n_tw
    lanes = 2 * GROUP if own_width % (2 * GROUP) == 0 else own_width
    chunks = own_width // lanes
    wide = min(n_tw, 2 * -(-HALO // tile_cols) + 1)

    flat = lanes % GROUP == 0

    q = queries.transpose(0, 2, 1, 3).reshape(tokens, model_width)
    kv = video_kv.transpose(0, 1, 3, 2, 4).reshape(2, tokens, model_width)
    out_form = (tokens, model_width)
    if not flat:
        q = q.reshape(tokens, n_tw, chunks, lanes).transpose(1, 2, 0, 3)
        kv = kv.reshape(2, tokens, n_tw, chunks, lanes).transpose(2, 3, 0, 1, 4)
        out_form = (n_tw, chunks, tokens, lanes)

    ids = np.arange(tokens)
    q_col, q_row = ids // tile_rows % tile_cols, ids % tile_rows
    q_meta = np.stack([q_row, q_col], axis=1).astype(np.int32)
    h_ids = np.arange(halo)
    h_block, h_row = h_ids // rows, h_ids % rows
    k_row = np.concatenate([h_row - rows, q_row, h_row + tile_rows])
    k_col = np.concatenate([h_block % tile_cols, q_col, h_block % tile_cols])
    band = np.floor_divide(k_row, tile_rows) + 1
    k_meta = np.zeros((8, span), np.int32)
    k_meta[0], k_meta[1] = k_row, band
    k_meta[2], k_meta[3] = k_row - (band - 1) * tile_rows, k_col
    picks = np.concatenate([h_block * tile_rows + h_row, h_block * tile_rows + h_row + tile_rows - rows])
    perm = (picks[:, None] == ids[None, :]).astype(np.float32)
    depth = GROUP if time_embed.shape[0] % GROUP == 0 else time_embed.shape[0]

    hbm = pl.BlockSpec(memory_space=pltpu.HBM)
    others = max(n_tw - 1, 1)
    dma = pltpu.SemaphoreType.DMA
    out = pl.pallas_call(
        functools.partial(kernel, (n_th, n_tw, chunks, lanes, tokens, halo, tile_cols, wide, flat)),
        out_shape=pltpu.VMEM(out_form, jnp.bfloat16),
        in_specs=[hbm] * 10,
        out_specs=hbm,
        scratch_shapes=[
            pltpu.SMEM((2, window_extent.shape[0]), jnp.int32),
            pltpu.SMEM((n_tw, 2, n_th), jnp.int32),
            pltpu.VMEM((time_embed.shape[0] // depth, depth), jnp.bfloat16),
            pltpu.VMEM(q_meta.shape, jnp.int32),
            pltpu.VMEM(k_meta.shape, jnp.int32),
            pltpu.VMEM(perm.shape, jnp.bfloat16),
            pltpu.VMEM((chunks, n_tw, tokens, lanes), jnp.bfloat16),
            pltpu.VMEM((chunks, n_tw, 2, span, lanes), jnp.bfloat16),
            pltpu.VMEM((chunks, n_tw, 2, 2 * halo, lanes), jnp.bfloat16),
            pltpu.VMEM((chunks, n_tw, tokens, lanes), jnp.bfloat16),
            pltpu.VMEM((text_kv.shape[1], 2, text_kv.shape[2]), jnp.bfloat16),
            pltpu.VMEM((chunks, 2, -(-text_kv.shape[1] // GROUP) * GROUP, lanes), jnp.bfloat16),
            pltpu.VMEM(gate_weight.shape, jnp.bfloat16),
            pltpu.VMEM((chunks, 1, lanes), jnp.float32),
            pltpu.VMEM((n_tw, HALO * HALO, tokens, wide * span), jnp.float32),
            dma((1,)),
            dma((others,)),
            pltpu.VMEM((tokens, lanes), jnp.bfloat16),
        ],
        compiler_params=pltpu.CompilerParams(
            collective_id=0, has_side_effects=True, vmem_limit_bytes=56 * 1024 * 1024
        ),
    )(
        window_extent.T,
        tile_valid.transpose(1, 2, 0),
        q,
        kv,
        text_kv.transpose(1, 0, 2),
        time_embed.reshape(-1, depth),
        gate_weight,
        jnp.asarray(q_meta),
        jnp.asarray(k_meta),
        jnp.asarray(perm, jnp.bfloat16),
    )
    if not flat:
        out = out.transpose(2, 0, 1, 3)
    return out.reshape(frames, tile_cols, tile_rows, model_width).transpose(0, 2, 1, 3)


def solution(mesh):
    placed = (
        P("vid", "th", "tw", None),
        P(None, "vid", "th", "tw", None),
        P(None, "vid", "tw"),
        P("vid"),
        P(None, "tw"),
        P(),
        P("vid", None, None),
    )
    return jax.shard_map(
        functools.partial(body, (mesh.shape["th"], mesh.shape["tw"])),
        mesh=mesh,
        in_specs=placed,
        out_specs=P("vid", "th", "tw", None),
        check_vma=False,
    )
```

```python
import functools

import jax
import jax.numpy as jnp
import numpy as np
from jax import lax
from jax.experimental import pallas as pl
from jax.experimental.pallas import tpu as pltpu
from jax.sharding import PartitionSpec as P

HEAD_DIM = 64
HALO = 3
NEG = -1e30
FAR = 1 << 20
GROUP = 128
MESH = pl.DeviceIdType.MESH


def halo_rows(tile_rows, per_row):
    for rows in range(HALO, tile_rows + 1):
        if rows * per_row % 16 == 0:
            return rows
    return tile_rows


def dot_nt(a, b):
    return lax.dot_general(a, b, (((1,), (1,)), ((), ())), preferred_element_type=jnp.float32)


def kernel(
    dims,
    ext_in,
    valid_in,
    q_in,
    kv_in,
    text_in,
    time_in,
    gw_in,
    qmeta_in,
    kmeta_in,
    perm_in,
    out_ref,
    ext_ref,
    valid_ref,
    time_ref,
    qmeta,
    kmeta,
    perm,
    qbuf,
    kvbuf,
    packed,
    obuf,
    text_raw,
    text_ref,
    gw_ref,
    gate,
    window,
    done_sem,
    out_recv,
    held,
):
    n_th, n_tw, chunks, lanes, tokens, halo, tile_cols, wide, flat = dims
    th = lax.axis_index("th")
    tw = lax.axis_index("tw")
    own = pl.ds(halo, tokens)
    has_up = th > 0
    has_down = th < n_th - 1
    others = max(n_tw - 1, 1)
    dma = pltpu.SemaphoreType.DMA

    def all_of(ref, sem):
        pltpu.make_async_copy(ref, ref, sem).wait()

    behind = max(chunks - 3, 0)
    lag = min(2, chunks)
    early = max(0, chunks - 1 - lag)
    detour = n_tw == 2 and n_th >= 4 and early > 2 and chunks > behind + 1
    turn = 2
    astray = chunks - 1 - behind

    def gather_and_attend(load_sem, kv_recv, q_recv, halo_recv, held_recv):
        span = tokens + 2 * halo
        heads_per_chunk = lanes // HEAD_DIM

        def peer(i):
            return lax.rem(tw + i, n_tw)

        def source(i):
            return lax.rem(tw + n_tw - i, n_tw)

        def piece(ref, j, c):
            if flat:
                return ref.at[..., pl.ds(pl.multiple_of((j * chunks + c) * lanes, lanes), lanes)]
            return ref.at[j, c]

        def remote(src, dst, ssem, rsem, where):
            return pltpu.make_async_remote_copy(
                src_ref=src, dst_ref=dst, send_sem=ssem, recv_sem=rsem, device_id=where, device_id_type=MESH
            )

        def kv_copy(c, i, slot):
            return remote(
                piece(kv_in, peer(i), c), kvbuf.at[c, slot, :, own, :], done_sem.at[0], kv_recv.at[c, i - 1], {"tw": peer(i)}
            )

        def q_copy(c, i, slot):
            return remote(
                piece(q_in, peer(i), c), qbuf.at[c, slot], done_sem.at[0], q_recv.at[c, i - 1], {"tw": peer(i)}
            )

        def kv_local(c):
            return pltpu.make_async_copy(piece(kv_in, tw, c), kvbuf.at[c, tw, :, own, :], load_sem.at[1])

        def q_local(c):
            return pltpu.make_async_copy(piece(q_in, tw, c), qbuf.at[c, tw], load_sem.at[1])

        def halo_up(c):
            dst = pl.ds(halo + tokens, halo)
            return remote(
                packed.at[c, :, :, pl.ds(0, halo), :], kvbuf.at[c, :, :, dst, :], done_sem.at[0], halo_recv.at[c], {"th": th - 1}
            )

        def halo_down(c):
            dst = pl.ds(0, halo)
            return remote(
                packed.at[c, :, :, pl.ds(halo, halo), :], kvbuf.at[c, :, :, dst, :], done_sem.at[0], halo_recv.at[c], {"th": th + 1}
            )

        def out_copy(c, i, slot):
            return remote(obuf.at[c, peer(i)], piece(out_ref, slot, c), done_sem.at[0], out_recv.at[i - 1], {"tw": peer(i)})

        def detour_copy():
            return remote(
                piece(q_in, peer(1), astray), held, done_sem.at[0], held_recv.at[0], {"th": turn, "tw": peer(1)}
            )

        def detour_last():
            return remote(held, qbuf.at[astray, peer(1)], done_sem.at[0], q_recv.at[astray, 0], {"th": 0})

        def out_local(c):
            return pltpu.make_async_copy(obuf.at[c, tw], piece(out_ref, tw, c), done_sem.at[0])

        barrier = pltpu.get_barrier_semaphore()
        for i in range(1, n_tw):
            pl.semaphore_signal(barrier, inc=1, device_id={"tw": peer(i)}, device_id_type=MESH)

        @pl.when(has_up)
        def _():
            pl.semaphore_signal(barrier, inc=1, device_id={"th": th - 1}, device_id_type=MESH)

        @pl.when(has_down)
        def _():
            pl.semaphore_signal(barrier, inc=1, device_id={"th": th + 1}, device_id_type=MESH)

        gw_load = pltpu.make_async_copy(gw_in, gw_ref, load_sem.at[0])
        text_load = pltpu.make_async_copy(text_in, text_raw, load_sem.at[1])
        for c in range(chunks):
            kv_local(c).start()
            q_local(c).start()
        small = [
            pltpu.make_async_copy(src, dst, load_sem.at[0])
            for src, dst in (
                [
                    (ext_in, ext_ref),
                    (valid_in, valid_ref),
                    (time_in, time_ref),
                    (qmeta_in, qmeta),
                    (kmeta_in, kmeta),
                    (perm_in, perm),
                ]
            )
        ]
        for load in small:
            load.start()
        gw_load.start()
        text_load.start()

        pl.semaphore_wait(barrier, n_tw - 1 + has_up.astype(jnp.int32) + has_down.astype(jnp.int32))

        for c in range(chunks + behind):
            for i in range(1, n_tw):
                if c < chunks:
                    kv_copy(c, i, tw).start()
                if c >= behind and not (detour and c - behind == astray):
                    q_copy(c - behind, i, tw).start()
            if detour and c - behind == astray:

                @pl.when(th != 0)
                def _():
                    q_copy(astray, 1, tw).start()

        @pl.when(jnp.logical_not(has_up))
        def _():
            kvbuf[:, :, :, pl.ds(0, halo), :] = jnp.zeros((chunks, n_tw, 2, halo, lanes), kvbuf.dtype)

        @pl.when(jnp.logical_not(has_down))
        def _():
            kvbuf[:, :, :, pl.ds(halo + tokens, halo), :] = jnp.zeros((chunks, n_tw, 2, halo, lanes), kvbuf.dtype)

        def find_gate():
            time = time_ref[...].astype(jnp.float32)
            mod_in = (time / (1.0 + jnp.exp(-time))).astype(jnp.bfloat16)
            depth = mod_in.shape[1]
            gate_vec = jnp.zeros((1, chunks * lanes), jnp.float32)
            for k in range(mod_in.shape[0]):
                gate_vec = gate_vec + jnp.dot(
                    mod_in[k : k + 1], gw_ref[k * depth : (k + 1) * depth], preferred_element_type=jnp.float32
                )
            gate_vec = gate_vec.astype(jnp.bfloat16).astype(jnp.float32)
            for c in range(chunks):
                gate[c] = gate_vec[:, c * lanes : (c + 1) * lanes]

        for load in small:
            load.wait()
        gw_load.wait()

        reach = -(-HALO // tile_cols)

        def first_tile(t):
            return jnp.clip(t - reach, 0, n_tw - wide)

        q_row = qmeta[:, 0:1]
        q_col = qmeta[:, 1:2]
        k_row = kmeta[0:1, :]
        k_band = kmeta[1:2, :]
        k_local = kmeta[2:3, :]
        k_col = kmeta[3:4, :]
        above = jnp.maximum(th - 1, 0)
        below = jnp.minimum(th + 1, n_th - 1)

        def windows(t, carry):
            start = first_tile(t)
            for j in range(wide):
                tc = start + j
                limits = []
                for what in range(2):
                    up = jnp.where(has_up, valid_ref[tc, what, above], 0)
                    mid = valid_ref[tc, what, th]
                    down = jnp.where(has_down, valid_ref[tc, what, below], 0)
                    limits.append(jnp.where(k_band == 0, up, jnp.where(k_band == 1, mid, down)))
                bad = jnp.where((k_local < limits[0]) & (k_col < limits[1]), 0, FAR)
                row_gap = jnp.abs(k_row - q_row) + bad
                col_gap = jnp.abs(k_col + (tc - t) * tile_cols - q_col)
                for r in range(HALO):
                    near = row_gap <= r + 1
                    for k in range(HALO):
                        window[t, r * HALO + k, :, pl.ds(j * span, span)] = jnp.where(near & (col_gap <= k + 1), 0.0, NEG)
            return carry

        lax.fori_loop(0, n_tw, windows, 0)
        find_gate()
        text_load.wait()
        texts = text_raw.shape[0]
        padded = text_ref.shape[2]
        if padded > texts:
            text_ref[:, :, texts // 16 * 16 :, :] = jnp.zeros((chunks, 2, padded - texts // 16 * 16, lanes), text_ref.dtype)

        video = wide * span
        beyond = texts // GROUP * GROUP

        def attend(c, t):
            start = first_tile(t)
            q_ok = (q_row < valid_ref[t, 0, th]) & (q_col < valid_ref[t, 1, th])
            tail = lax.broadcasted_iota(jnp.int32, (1, padded - beyond), 1) + beyond
            tail_bias = jnp.where(tail < texts, 0.0, NEG)
            for low in range(0, lanes, GROUP):
                width = min(GROUP, lanes - low)
                count = width // HEAD_DIM
                part = pl.ds(low, width)
                q = qbuf[c, t, :, part]
                keys, values = [
                    jnp.concatenate(
                        [kvbuf[c, pl.ds(start, wide), s, :, part].reshape(video, width), text_ref[c, s, :, part]], axis=0
                    )
                    for s in range(2)
                ]
                lane = lax.broadcasted_iota(jnp.int32, (1, width), 1)
                stacked = []
                for s in range(count):
                    mine = (lane >= s * HEAD_DIM) & (lane < (s + 1) * HEAD_DIM)
                    stacked.append(q * jnp.where(mine, HEAD_DIM ** -0.5, 0.0).astype(jnp.bfloat16))
                q_all = jnp.concatenate(stacked, axis=0) if count > 1 else stacked[0]
                scores = dot_nt(q_all, keys)
                weights, inverse = [], []
                for s in range(count):
                    head = tw * (chunks * heads_per_chunk) + c * heads_per_chunk + low // HEAD_DIM + s
                    reach_at = (jnp.clip(ext_ref[0, head], 1, HALO) - 1) * HALO + jnp.clip(ext_ref[1, head], 1, HALO) - 1
                    mine = scores[s * tokens : (s + 1) * tokens]
                    pieces = [mine[:, :video] + window[t, reach_at]]
                    if beyond:
                        pieces.append(mine[:, video : video + beyond])
                    if padded > beyond:
                        pieces.append(mine[:, video + beyond :] + tail_bias)
                    near = jnp.concatenate(pieces, axis=1)
                    top = jnp.max(near, axis=-1, keepdims=True)
                    e = jnp.exp(near - top)
                    inverse.append(1.0 / jnp.sum(e, axis=-1, keepdims=True))
                    weights.append(e.astype(jnp.bfloat16))
                w_all = jnp.concatenate(weights, axis=0) if count > 1 else weights[0]
                mixed = jnp.dot(w_all, values, preferred_element_type=jnp.float32)
                result = mixed[0:tokens] * inverse[0]
                for s in range(1, count):
                    result = jnp.where(lane >= s * HEAD_DIM, mixed[s * tokens : (s + 1) * tokens] * inverse[s], result)
                result = result * gate[c, :, part]
                obuf[c, t, :, part] = jnp.where(q_ok, result, 0.0).astype(jnp.bfloat16)

        def halos_here(c):
            @pl.when(has_down & has_up)
            def _():
                all_of(packed.at[c], halo_recv.at[c])

            @pl.when(has_down != has_up)
            def _():
                all_of(packed.at[c, :, :, pl.ds(0, halo), :], halo_recv.at[c])

        all_of(kvbuf.at[:, tw, :, own, :], load_sem.at[1])
        all_of(qbuf.at[:, tw], load_sem.at[1])

        def step(at, carry):
            if detour:

                @pl.when((th == turn) & (at == lag + early - 1))
                def _():
                    all_of(held, held_recv.at[0])
                    detour_last().start()

            @pl.when(at < chunks)
            def _():
                for i in range(1, n_tw):
                    kv_copy(at, i, source(i)).wait_recv()

                def pack(j, inner):
                    for s in range(2):
                        rows = jnp.dot(perm[...], kvbuf[at, j, s, own, :], preferred_element_type=jnp.float32)
                        packed[at, j, s] = rows.astype(jnp.bfloat16)
                    return inner

                lax.fori_loop(0, n_tw, pack, 0)

                @pl.when(has_up)
                def _():
                    halo_up(at).start()

                @pl.when(has_down)
                def _():
                    halo_down(at).start()

            @pl.when((at >= lag) & (at < lag + early))
            def _():
                halos_here(at - lag)

            if detour:

                @pl.when((th == 0) & (at == lag))
                def _():
                    detour_copy().start()

            @pl.when(at < -(-chunks // 2))
            def _():
                for k in range(min(2, chunks)):
                    c = jnp.minimum(2 * at + k, chunks - 1)
                    mine = slice(None) if chunks == 1 else pl.ds(pl.multiple_of(c * lanes, lanes), lanes)
                    for s in range(2):
                        text_ref[c, s, :texts] = text_raw[:, s, mine]

            late = at >= chunks + behind
            own_now = ((at >= lag) & (at < lag + early)) | late
            away_now = (at >= behind) & jnp.logical_not(late)
            own_c = jnp.where(late, at - (chunks + behind) + early, at - lag)
            away_c = at - behind

            def job(i, inner):
                home = i == 0
                c = jnp.where(home, own_c, away_c)

                @pl.when((i == 1) & (c >= early))
                def _():
                    halos_here(c)

                @pl.when(jnp.logical_not(home))
                def _():
                    q_copy(c, n_tw - i, peer(i)).wait_recv()

                attend(c, peer(i))

                @pl.when(home)
                def _():
                    out_local(c).start()

                @pl.when(jnp.logical_not(home))
                def _():
                    out_copy(c, i, tw).start()

                return inner

            lax.fori_loop(jnp.where(own_now, 0, 1), jnp.where(away_now, n_tw, 1), job, 0)
            return carry

        lax.fori_loop(0, 2 * chunks + behind - early, step, 0)

    pl.run_scoped(
        gather_and_attend,
        dma((2,)),
        dma((chunks, others)),
        dma((chunks, others)),
        dma((chunks,)),
        dma((1,)),
    )

    for i in range(1, n_tw):
        all_of(kvbuf.at[:, tw, :, own, :], done_sem.at[0])
        all_of(qbuf.at[:, tw], done_sem.at[0])
        all_of(obuf.at[:, tw], done_sem.at[0])
    all_of(obuf.at[:, tw], done_sem.at[0])

    if detour:

        @pl.when(th == turn)
        def _():
            all_of(held, done_sem.at[0])

    @pl.when(has_up)
    def _():
        all_of(packed.at[:, :, :, pl.ds(0, halo), :], done_sem.at[0])

    @pl.when(has_down)
    def _():
        all_of(packed.at[:, :, :, pl.ds(halo, halo), :], done_sem.at[0])

    for i in range(1, n_tw):
        all_of(obuf.at[:, tw], out_recv.at[i - 1])


def body(sizes, queries, video_kv, text_kv, time_embed, gate_weight, window_extent, tile_valid):
    n_th, n_tw = sizes
    frames, tile_rows, tile_cols, model_width = queries.shape
    per_row = frames * tile_cols
    tokens = tile_rows * per_row
    rows = halo_rows(tile_rows, per_row)
    halo = rows * per_row
    span = tokens + 2 * halo
    own_width = model_width // n_tw
    lanes = 2 * GROUP if own_width % (2 * GROUP) == 0 else own_width
    chunks = own_width // lanes
    wide = min(n_tw, 2 * -(-HALO // tile_cols) + 1)

    flat = lanes % GROUP == 0

    q = queries.transpose(0, 2, 1, 3).reshape(tokens, model_width)
    kv = video_kv.transpose(0, 1, 3, 2, 4).reshape(2, tokens, model_width)
    out_form = (tokens, model_width)
    if not flat:
        q = q.reshape(tokens, n_tw, chunks, lanes).transpose(1, 2, 0, 3)
        kv = kv.reshape(2, tokens, n_tw, chunks, lanes).transpose(2, 3, 0, 1, 4)
        out_form = (n_tw, chunks, tokens, lanes)

    ids = np.arange(tokens)
    q_col, q_row = ids // tile_rows % tile_cols, ids % tile_rows
    q_meta = np.stack([q_row, q_col], axis=1).astype(np.int32)
    h_ids = np.arange(halo)
    h_block, h_row = h_ids // rows, h_ids % rows
    k_row = np.concatenate([h_row - rows, q_row, h_row + tile_rows])
    k_col = np.concatenate([h_block % tile_cols, q_col, h_block % tile_cols])
    band = np.floor_divide(k_row, tile_rows) + 1
    k_meta = np.zeros((8, span), np.int32)
    k_meta[0], k_meta[1] = k_row, band
    k_meta[2], k_meta[3] = k_row - (band - 1) * tile_rows, k_col
    picks = np.concatenate([h_block * tile_rows + h_row, h_block * tile_rows + h_row + tile_rows - rows])
    perm = (picks[:, None] == ids[None, :]).astype(np.float32)
    depth = GROUP if time_embed.shape[0] % GROUP == 0 else time_embed.shape[0]

    hbm = pl.BlockSpec(memory_space=pltpu.HBM)
    others = max(n_tw - 1, 1)
    dma = pltpu.SemaphoreType.DMA
    out = pl.pallas_call(
        functools.partial(kernel, (n_th, n_tw, chunks, lanes, tokens, halo, tile_cols, wide, flat)),
        out_shape=pltpu.VMEM(out_form, jnp.bfloat16),
        in_specs=[hbm] * 10,
        out_specs=hbm,
        scratch_shapes=[
            pltpu.SMEM((2, window_extent.shape[0]), jnp.int32),
            pltpu.SMEM((n_tw, 2, n_th), jnp.int32),
            pltpu.VMEM((time_embed.shape[0] // depth, depth), jnp.bfloat16),
            pltpu.VMEM(q_meta.shape, jnp.int32),
            pltpu.VMEM(k_meta.shape, jnp.int32),
            pltpu.VMEM(perm.shape, jnp.bfloat16),
            pltpu.VMEM((chunks, n_tw, tokens, lanes), jnp.bfloat16),
            pltpu.VMEM((chunks, n_tw, 2, span, lanes), jnp.bfloat16),
            pltpu.VMEM((chunks, n_tw, 2, 2 * halo, lanes), jnp.bfloat16),
            pltpu.VMEM((chunks, n_tw, tokens, lanes), jnp.bfloat16),
            pltpu.VMEM((text_kv.shape[1], 2, text_kv.shape[2]), jnp.bfloat16),
            pltpu.VMEM((chunks, 2, -(-text_kv.shape[1] // GROUP) * GROUP, lanes), jnp.bfloat16),
            pltpu.VMEM(gate_weight.shape, jnp.bfloat16),
            pltpu.VMEM((chunks, 1, lanes), jnp.float32),
            pltpu.VMEM((n_tw, HALO * HALO, tokens, wide * span), jnp.float32),
            dma((1,)),
            dma((others,)),
            pltpu.VMEM((tokens, lanes), jnp.bfloat16),
        ],
        compiler_params=pltpu.CompilerParams(
            collective_id=0, has_side_effects=True, vmem_limit_bytes=56 * 1024 * 1024
        ),
    )(
        window_extent.T,
        tile_valid.transpose(1, 2, 0),
        q,
        kv,
        text_kv.transpose(1, 0, 2),
        time_embed.reshape(-1, depth),
        gate_weight,
        jnp.asarray(q_meta),
        jnp.asarray(k_meta),
        jnp.asarray(perm, jnp.bfloat16),
    )
    if not flat:
        out = out.transpose(2, 0, 1, 3)
    return out.reshape(frames, tile_cols, tile_rows, model_width).transpose(0, 2, 1, 3)


def solution(mesh):
    placed = (
        P("vid", "th", "tw", None),
        P(None, "vid", "th", "tw", None),
        P(None, "vid", "tw"),
        P("vid"),
        P(None, "tw"),
        P(),
        P("vid", None, None),
    )
    return jax.shard_map(
        functools.partial(body, (mesh.shape["th"], mesh.shape["tw"])),
        mesh=mesh,
        in_specs=placed,
        out_specs=P("vid", "th", "tw", None),
        check_vma=False,
    )
```
